32 devices in a mesh: gx: 8 (over z, x), gy: 4 (over y, core).
Axes of the slice: x: 2, y: 2, z: 4, core: 2. Of those that a mesh axis runs over, the one named last changes fastest.
Arguments:
- state: float32 [65536, 128], P(('gx', 'gy')), may hold values from 0 to 1
- velocity: bfloat16 [3, 3, 128, 64, 128], P(None, None, 'gx', 'gy'), may hold values from -3 to 3
- cells: int32 [3, 3, 65536], P(None, None, ('gx', 'gy')), may hold values from -1 to 126, as said below
- slots: int32 [3, 65536], P(None, ('gx', 'gy')), may hold values from 0 to 2047, as said below
- counts: int32 [3, 8, 4, 8], P(None, 'gx', 'gy'), may hold values from 0 to 64, as said below
Outputs:
- final_state: float32 [65536, 128], P(('gx', 'gy'))
The draws below stay inside these ranges and needn't reach their ends.
Inputs may be any that keep to these rules, and one draw needn't show every extreme that they name: For every section and device the 2048 values of slots are a permutation of 0 to 2047. counts[s, i, j, r] equals counts[s, i', j', r xor 1] where (i', j') is the neighbour of (i, j) in direction r; some device sends exactly 64 in every section. cells[s, 0] lies in -1 to 15, cells[s, 1] in -1 to 15, cells[s, 2] in 0 to 126.
All inputs are finite; a program needn't handle non-finite values.
Results may differ from the reference program's by a relative error of at most 0.0003.
Values may be sent and summed in bfloat16 or wider, within the bound.
A program may use at most 64 MiB of HBM per device.

```python
import jax
import jax.numpy as jnp

CX = 16
CY = 16
NZ = 128
PART_DEV = 2048
CAP = 64
S = 128
SECTIONS = 3
NX = 128
NY = 64
NPART = 65536
N_GX = 8
N_GY = 4


def draw_counts(key, part):
    forward = jax.random.randint(key, (SECTIONS, N_GX, N_GY, 4), CAP // 4, CAP + 1)
    picks = jax.random.randint(jax.random.fold_in(key, 7), (SECTIONS,), 0, N_GX * N_GY)
    hot = (jnp.arange(N_GX * N_GY)[None, :] == picks[:, None]).reshape(SECTIONS, N_GX, N_GY)
    east = jnp.where(hot, CAP, forward[..., 0])
    north = forward[..., 1]
    rising = forward[..., 2]
    falling = forward[..., 3]
    table = jnp.stack([east, jnp.roll(east, 1, axis=1), north, jnp.roll(north, 1, axis=2), rising, jnp.roll(rising, (1, 1), axis=(1, 2)), falling, jnp.roll(falling, (1, -1), axis=(1, 2))], axis=-1)
    return table.astype(jnp.int32)


def draw_slots(key, part):
    scores = jax.random.randint(key, (SECTIONS, N_GX * N_GY, PART_DEV), 0, 2 ** 18)
    scores = scores * PART_DEV + jnp.arange(PART_DEV, dtype=jnp.int32)[None, None, :]
    order = jnp.argsort(scores, axis=-1, stable=True).astype(jnp.int32)
    return order.reshape(SECTIONS, N_GX * N_GY * PART_DEV)


def draw_cells(key, part):
    npart = N_GX * N_GY * PART_DEV
    cell_x = jax.random.randint(jax.random.fold_in(key, 1), (SECTIONS, npart), -1, CX)
    cell_y = jax.random.randint(jax.random.fold_in(key, 2), (SECTIONS, npart), -1, CY)
    cell_z = jax.random.randint(jax.random.fold_in(key, 3), (SECTIONS, npart), 0, NZ - 1)
    return jnp.stack([cell_x, cell_y, cell_z], axis=1).astype(jnp.int32)


def level_of(key, shape, split, low, top_value):
    gain = 1.0
    for position, parts in split:
        draws = jax.random.uniform(jax.random.fold_in(jax.random.fold_in(key, 6), position), (parts,), jnp.float32, low / len(split), top_value / len(split))
        gain = gain * jnp.repeat(jnp.exp(draws), shape[position] // parts).reshape((-1,) + (1,) * (len(shape) - 1 - position))
    return gain


def normal_values(own_key, dims, scale, reach, pieces=(), held_as=jnp.bfloat16):
    gain = level_of(own_key, dims, pieces, -0.22, 0.18) if pieces else 1.0
    array = jax.random.normal(own_key, dims, jnp.float32) * scale * gain
    return jnp.minimum(jnp.maximum(array, -reach), reach).astype(held_as)


def setup_inputs(seed: int = 0) -> dict:
    key_of = jax.random.split(jax.random.key(seed), 6)
    state = jnp.clip(1.0 * jax.random.uniform(key_of[0], (NPART, S), jnp.float32) ** level_of(key_of[0], (NPART, S), ((0, 32),), -0.2, 0.2), 0.0, 1.0)
    velocity = normal_values(key_of[1], (SECTIONS, 3, NX, NY, NZ), 0.4, 3.0, ((2, 8), (3, 4)))
    cells = draw_cells(jax.random.fold_in(key_of[5], 71), 0)
    slots = draw_slots(jax.random.fold_in(key_of[5], 71), 0)
    counts = draw_counts(jax.random.fold_in(key_of[5], 71), 0)
    return dict(state=state, velocity=velocity, cells=cells, slots=slots, counts=counts)


GAMMA = (8.0 / 15.0, 5.0 / 12.0, 3.0 / 4.0)
ZETA = (0.0, -17.0 / 60.0, -5.0 / 12.0)
OFFSETS = ((1, 0), (-1, 0), (0, 1), (0, -1), (1, 1), (-1, -1), (1, -1), (-1, 1))
OPPOSITE = (1, 0, 3, 2, 5, 4, 7, 6)


def reference(state, velocity, cells, slots, counts):
    devices = N_GX * N_GY
    npart = devices * PART_DEV
    owner = jnp.arange(npart, dtype=jnp.int32) // PART_DEV
    row_i = owner // N_GY
    col_j = owner % N_GY
    lanes = jnp.arange(devices, dtype=jnp.int32)
    lane_i = lanes // N_GY
    lane_j = lanes % N_GY
    within = jnp.arange(CAP, dtype=jnp.int32)
    for section in range(SECTIONS):
        field = velocity[section]
        base_x = row_i * CX + cells[section, 0]
        base_y = col_j * CY + cells[section, 1]
        base_z = cells[section, 2]
        frac = state[:, 0:3]
        sampled = jnp.zeros((3, npart), jnp.float32)
        for a in (0, 1):
            for b in (0, 1):
                for c in (0, 1):
                    weight_x = frac[:, 0] if a else 1.0 - frac[:, 0]
                    weight_y = frac[:, 1] if b else 1.0 - frac[:, 1]
                    weight_z = frac[:, 2] if c else 1.0 - frac[:, 2]
                    index_x = (base_x + a) % NX
                    index_y = (base_y + b) % NY
                    values = field[:, index_x, index_y, base_z + c].astype(jnp.float32)
                    sampled = sampled + (weight_x * weight_y * weight_z)[None, :] * values
        speed = sampled.T
        moved = frac + GAMMA[section] * speed + ZETA[section] * state[:, 3:6]
        state = jnp.concatenate([moved, speed, state[:, 6:]], axis=1)
        order = slots[section].reshape(devices, PART_DEV)
        tally = counts[section].reshape(devices, 8)
        source = jnp.arange(npart, dtype=jnp.int32)
        for direction in range(8):
            off_x, off_y = OFFSETS[direction]
            back = OPPOSITE[direction]
            neighbour = ((lane_i + off_x) % N_GX) * N_GY + (lane_j + off_y) % N_GY
            far = neighbour[:, None] * PART_DEV + order[neighbour, back * CAP:(back + 1) * CAP]
            near = lanes[:, None] * PART_DEV + order[:, direction * CAP:(direction + 1) * CAP]
            picked = jnp.where(within[None, :] < tally[:, direction:direction + 1], far, near)
            source = source.at[near.reshape(-1)].set(picked.reshape(-1).astype(jnp.int32))
        state = state[source]
    return state
```

```python
import functools

import jax
import jax.numpy as jnp
from jax import lax
from jax.experimental import pallas as pl
from jax.experimental.pallas import tpu as pltpu
from jax.sharding import PartitionSpec as P

GAMMA = (8.0 / 15.0, 5.0 / 12.0, 3.0 / 4.0)
ZETA = (0.0, -17.0 / 60.0, -5.0 / 12.0)
OFFSETS = ((1, 0), (-1, 0), (0, 1), (0, -1), (1, 1), (-1, -1), (1, -1), (-1, 1))
LANES = 128
SPARE = 8
BLOCK = 512
MESH = pl.DeviceIdType.MESH
VMEM = pl.BlockSpec(memory_space=pltpu.VMEM)
SMEM = pl.BlockSpec(memory_space=pltpu.SMEM)
ANY = pl.BlockSpec(memory_space=pl.ANY)


def neighbour(r, sizes):
    off_x, off_y = OFFSETS[r]
    i, j = lax.axis_index("gx"), lax.axis_index("gy")
    return (lax.rem(i + off_x + sizes[0], sizes[0]), lax.rem(j + off_y + sizes[1], sizes[1]))


def send(r, src, dst, sems, group, sizes):
    copy = pltpu.make_async_remote_copy(
        src_ref=src,
        dst_ref=dst,
        send_sem=sems[0].at[group, r],
        recv_sem=sems[1].at[group, r],
        device_id=neighbour(r, sizes),
        device_id_type=MESH,
    )
    copy.start()
    return copy


def tile(x, k):
    return x[:, k * LANES : (k + 1) * LANES]


def spread_row(row):
    return jnp.broadcast_to(row, (8, LANES))


def select_lanes(tiles, where_, start):
    low, high = where_ & (LANES - 1), where_ >> 7
    out = start
    for k, source in enumerate(tiles):
        out = jnp.where(high == k, jnp.take_along_axis(source, low, axis=1), out)
    return out


def look_up(table, where_):
    low, high = spread_row(where_ & (LANES - 1)), spread_row(where_ >> 7)
    row = lax.broadcasted_iota(jnp.int32, (8, LANES), 0)
    best = jnp.zeros((8, LANES), jnp.int32)
    for g in range(table.shape[0] // 8):
        got = jnp.take_along_axis(table[8 * g : 8 * g + 8], low, axis=1)
        best = jnp.where(row + 8 * g == high, got, best)
    return jnp.max(best, axis=0, keepdims=True)


def cell_weights(size, cell, frac):
    spots = lax.broadcasted_iota(jnp.int32, (size, cell.shape[1]), 0)
    low, high = 1.0 - frac, frac
    inside = jnp.where(spots == cell, low, jnp.where(spots == cell + 1, high, 0.0))
    return inside, jnp.where(cell == -1, low, 0.0), jnp.where(cell == size - 1, high, 0.0)


def halves(whole):
    high = whole.astype(jnp.bfloat16)
    return high, (whole - high.astype(jnp.float32)).astype(jnp.bfloat16)


def sample(section, dims, head, cell, plane_ref):
    cx, cy = dims
    inner = cx * cy
    depth = plane_ref.shape[0] // 3
    block = head.shape[1]
    wx, wx_low, wx_high = cell_weights(cx, cell[0:1], head[0:1])
    wy, wy_low, wy_high = cell_weights(cy, cell[1:2], head[1:2])
    wz, _, _ = cell_weights(depth, cell[2:3], head[2:3])
    own = jnp.concatenate([wx[x : x + 1] * wy for x in range(cx)], axis=0)
    rim = [wx_high * wy, wx_low * wy, wx * wy_high, wx * wy_low]
    rim += [wx_high * wy_high, wx_low * wy_low, wx_high * wy_low, wx_low * wy_high]
    rim += [jnp.zeros((LANES - 2 * cx - 2 * cy - 4, block), jnp.float32)]
    own_high, own_low = halves(own)
    rim = jnp.concatenate(halves(jnp.concatenate(rim, axis=0)), axis=0)
    inside = plane_ref[:, 0:inner]
    columns = jnp.dot(inside, own_high, preferred_element_type=jnp.float32)
    columns = columns + jnp.dot(inside, own_low, preferred_element_type=jnp.float32)
    columns = columns + jnp.dot(plane_ref[:, inner:], rim, preferred_element_type=jnp.float32)
    speed = jnp.concatenate(
        [jnp.sum(columns[k * depth : (k + 1) * depth] * wz, axis=0, keepdims=True) for k in range(3)],
        axis=0,
    )
    moved = head[0:3] + GAMMA[section] * speed + ZETA[section] * head[3:6]
    return jnp.concatenate([moved, speed, jnp.ones((2, block), jnp.float32)], axis=0)


def sample_all(section, dims, cells_ref, head_ref, plane_ref):
    block = BLOCK

    def body(step, carry):
        span = pl.ds(pl.multiple_of(step * block, block), block)
        head_ref[:, span] = sample(section, dims, head_ref[:, span], cells_ref[section, :, span], plane_ref)
        return carry

    lax.fori_loop(0, head_ref.shape[1] // block, body, 0)


def gather_rows(index_ref, section, source_ref, leave_ref):
    def body(row, carry):
        for u in range(LANES):
            leave_ref[section, pl.ds(row * LANES + u, 1), :] = source_ref[pl.ds(index_ref[section, row, u], 1), :]
        return carry

    lax.fori_loop(0, leave_ref.shape[1] // LANES, body, 0)


def find_edges(fields, dims, v_ref, yface_ref, away_ref):
    cx, cy = dims
    inner = cx * cy
    row = lax.broadcasted_iota(jnp.int32, (2 * cx + 8, inner), 0)
    place = lax.broadcasted_iota(jnp.int32, (2 * cx + 8, inner), 1)
    want = jnp.where(row < cx, row * cy + cy - 1, (row - cx) * cy)
    for d, spot in enumerate((inner - 1, 0, (cx - 1) * cy, cy - 1)):
        want = jnp.where(row == 2 * cx + d, spot, want)
    pick = jnp.where(want == place, 1.0, 0.0).astype(jnp.bfloat16)
    for f in fields:
        edge = jnp.dot(pick, v_ref[f].reshape(inner, v_ref.shape[3]), preferred_element_type=jnp.float32)
        yface_ref[0, f] = edge[0:cx].astype(jnp.bfloat16)
        yface_ref[1, f] = edge[cx : 2 * cx].astype(jnp.bfloat16)
        group, line = (0, f) if f < 3 else (1, f - 3)
        for d in range(4):
            away_ref[group, d, line : line + 1, :] = edge[2 * cx + d : 2 * cx + d + 1]


def build_inside(section, dims, v_ref, plane_ref):
    inner = dims[0] * dims[1]
    depth = v_ref.shape[3]
    for k in range(3):
        own = v_ref[3 * section + k].reshape(inner, depth)
        plane_ref[pl.ds(k * depth, depth), 0:inner] = own.T


def build_rim(section, dims, halo_ref, corner_ref, plane_ref):
    inner = dims[0] * dims[1]
    depth = halo_ref.shape[2]
    for k in range(3):
        f = 3 * section + k
        group, line = (0, f) if f < 3 else (1, f - 3)
        faces = halo_ref[f].astype(jnp.float32)
        corners = [corner_ref[group, d, line : line + 1, :] for d in range(4)]
        filler = jnp.zeros((LANES - faces.shape[0] - 4, depth), jnp.float32)
        edge = jnp.concatenate([faces] + corners + [filler], axis=0).T.astype(jnp.bfloat16)
        plane_ref[pl.ds(k * depth, depth), inner : inner + LANES] = edge
        plane_ref[pl.ds(k * depth, depth), inner + LANES :] = edge


def plan(section, cap, count, slots_ref, counts_ref):
    moving = 8 * cap
    blocks = count // LANES
    slot = slots_ref[section : section + 1, 0:moving]
    lanes = lax.broadcasted_iota(jnp.int32, (1, moving), 1)
    limit = jnp.zeros((1, moving), jnp.int32)
    for r in range(8):
        limit = jnp.where(lanes >= r * cap, counts_ref[section, 0, 0, r], limit)
    taken = lax.rem(lanes, cap) < limit
    goal = jnp.where(taken, slot, count)
    value = jnp.where(taken, (lanes ^ cap) + 1, 0)
    low, high = slot & (LANES - 1), slot >> 7
    line = lax.broadcasted_iota(jnp.int32, (blocks, moving), 0)
    upper = jnp.where(line == high, (value >> 5).astype(jnp.float32), 0.0)
    lower = jnp.where(line == high, (value & 31).astype(jnp.float32), 0.0)
    left = jnp.concatenate([upper, lower], axis=0).astype(jnp.bfloat16)
    spots = lax.broadcasted_iota(jnp.int32, (LANES, moving), 0)
    right = jnp.where(spots == low, 1.0, 0.0).astype(jnp.bfloat16)
    both = lax.dot_general(left, right, (((1,), (1,)), ((), ())), preferred_element_type=jnp.float32)
    inverse = (both[0:blocks] * 32.0 + both[blocks:]).astype(jnp.int32)
    return slot, goal, inverse


def steps_kernel(
    sizes,
    cap,
    state_hbm,
    v_hbm,
    cells_hbm,
    slots_hbm,
    counts_hbm,
    rows_ref,
    arrived_ref,
    head_ref,
    index_ref,
    counts_ref,
    v_ref,
    cells_ref,
    slots_ref,
    staged_ref,
    inverse_ref,
    from_ref,
    there_ref,
    own_ref,
    leave_ref,
    plane_ref,
    yface_ref,
    away_ref,
    halo_ref,
    corner_ref,
    head_out_ref,
    head_in_ref,
    local_sem,
    send_sem,
    recv_sem,
):
    sems = (send_sem, recv_sem)
    sections, _, count = cells_ref.shape
    cx, cy = v_ref.shape[1], v_ref.shape[2]
    dims = (cx, cy)
    moving = 8 * cap
    chunks = moving // LANES
    blocks = count // LANES
    fields = 3 * sections
    starts = (0, cy, 2 * cy, 2 * cy + cx)
    widths = (cy, cy, cx, cx)

    barrier = pltpu.get_barrier_semaphore()
    for r in range(8):
        pl.semaphore_signal(barrier, inc=1, device_id=neighbour(r, sizes), device_id_type=MESH)

    def fetch(k, src, dst):
        copy = pltpu.make_async_copy(src, dst, local_sem.at[k])
        copy.start()
        return copy

    load_first = fetch(0, v_hbm.at[pl.ds(0, 3)], v_ref.at[pl.ds(0, 3)])
    load_slots = fetch(1, slots_hbm, slots_ref)
    load_counts = fetch(2, counts_hbm, counts_ref)
    load_state = fetch(3, state_hbm, rows_ref.at[pl.ds(0, count)])
    load_cells = fetch(4, cells_hbm, cells_ref)
    load_rest = fetch(5, v_hbm.at[pl.ds(3, fields - 3)], v_ref.at[pl.ds(3, fields - 3)])

    def send_halo(group):
        span = pl.ds(0, 3) if group == 0 else pl.ds(3, fields - 3)
        copies = []
        for r in range(8):
            if r < 4:
                off_x, off_y = OFFSETS[r]
                src = v_ref.at[span, cx - 1 if off_x > 0 else 0] if off_x else yface_ref.at[r - 2, span]
                dst = halo_ref.at[span, pl.ds(starts[r ^ 1], widths[r ^ 1]), :]
            else:
                src, dst = away_ref.at[group, r - 4], corner_ref.at[group, (r ^ 1) - 4]
            copies.append(send(r, src, dst, sems, group, sizes))
        return copies

    load_first.wait()
    find_edges(range(3), dims, v_ref, yface_ref, away_ref)
    pl.semaphore_wait(barrier, 8)
    halos = [send_halo(0)]

    load_slots.wait()
    load_counts.wait()
    slots, inverses = [], []
    table = lax.broadcasted_iota(jnp.int32, (blocks, LANES), 0) * LANES
    table = table + lax.broadcasted_iota(jnp.int32, (blocks, LANES), 1)
    places = []
    for section in range(sections):
        slot, goal, inverse = plan(section, cap, count, slots_ref, counts_ref)
        if section:
            packed = table * 1024 + inverses[-1]
            found = [look_up(packed, tile(slot, c)) for c in range(chunks)]
            for c in range(chunks):
                staged_ref[section, c : c + 1, :] = jnp.clip(found[c] >> 10, 0, count + section * moving - 1)
                from_ref[section, c : c + 1, :] = (found[c] & 1023) - 1
        else:
            for c in range(chunks):
                staged_ref[section, c : c + 1, :] = tile(slot, c)
        for c in range(chunks):
            staged_ref[section, chunks + c : chunks + c + 1, :] = tile(goal, c)
        places.append(fetch(6 + section, staged_ref.at[section], index_ref.at[section]))
        table = jnp.where(inverse > 0, inverse + (count + section * moving - 1), table)
        inverse_ref[section] = inverse - 1
        slots.append(slot)
        inverses.append(inverse)

    load_rest.wait()
    find_edges(range(3, fields), dims, v_ref, yface_ref, away_ref)
    halos.append(send_halo(1))

    def send_rows(section):
        places[section].wait()
        gather_rows(index_ref, section, rows_ref, leave_ref)
        return [
            send(
                r,
                leave_ref.at[section, pl.ds(r * cap, cap)],
                arrived_ref.at[pl.ds(section * moving + r * cap, cap)],
                sems,
                2 + section,
                sizes,
            )
            for r in range(8)
        ]

    load_state.wait()
    carried = [send_rows(0)]
    build_inside(0, dims, v_ref, plane_ref.at[0])
    for b in range(blocks):
        head_ref[:, b * LANES : (b + 1) * LANES] = rows_ref[b * LANES : (b + 1) * LANES, :].T[0:8]

    load_cells.wait()
    line = lax.broadcasted_iota(jnp.int32, (8, LANES), 0)
    packed = []
    for b in range(blocks):
        span = slice(b * LANES, (b + 1) * LANES)
        both = jnp.zeros((8, LANES), jnp.int32)
        for section in range(sections):
            spot = cells_ref[section, :, span]
            word = (spot[0:1] + 1) + (spot[1:2] + 1) * 1024 + spot[2:3] * 1048576
            both = jnp.where(line == section, spread_row(word), both)
        packed.append(both)
    for c in range(chunks):
        where_ = spread_row(tile(slots[0], c))
        for section in range(1, sections):
            where_ = jnp.where(line == section, spread_row(tile(slots[section], c)), where_)
        there_ref[c] = select_lanes(packed, where_, jnp.zeros((8, LANES), jnp.int32))

    def pick_own(section):
        tiles = [head_ref[:, b * LANES : (b + 1) * LANES] for b in range(blocks)]
        for c in range(chunks):
            where_ = spread_row(slots_ref[section : section + 1, c * LANES : (c + 1) * LANES])
            own_ref[c] = select_lanes(tiles, where_, jnp.zeros((8, LANES), jnp.float32))

    def arrivals(section):
        first = lax.broadcasted_iota(jnp.int32, (8, LANES), 1) < cap
        return [
            jnp.where(first, head_in_ref[section, 2 * c], head_in_ref[section, 2 * c + 1]) for c in range(chunks)
        ]

    pick_own(0)
    heads = []
    for section in range(sections):
        if section == 0:
            for copy in halos[0]:
                copy.wait_recv()
            build_rim(0, dims, halo_ref, corner_ref, plane_ref.at[0])
            leaving = [own_ref[c] for c in range(chunks)]
        else:
            for copy in heads[section - 1]:
                copy.wait_recv()
            came = arrivals(section - 1)
            leaving = [
                select_lanes(came, spread_row(from_ref[section, c : c + 1, :]), own_ref[c]) for c in range(chunks)
            ]
        word = jnp.concatenate([there_ref[c, section : section + 1, :] for c in range(chunks)], axis=1)
        spot = jnp.concatenate([(word & 1023) - 1, ((word >> 10) & 1023) - 1, word >> 20], axis=0)
        leaving = sample(section, dims, jnp.concatenate(leaving, axis=1), spot, plane_ref.at[section])
        for c in range(chunks):
            head_out_ref[section, c] = tile(leaving, c)
        heads.append(
            [
                send(r, head_out_ref.at[section, r // 2], head_in_ref.at[section, r], sems, 2 + sections + section, sizes)
                for r in range(8)
            ]
        )

        if section:
            place_arrivals(section - 1, arrivals(section - 1), inverse_ref, head_ref)
        sample_all(section, dims, cells_ref, head_ref, plane_ref.at[section])
        if section + 1 < sections:
            pick_own(section + 1)
            build_inside(section + 1, dims, v_ref, plane_ref.at[section + 1])
            if section == 0:
                for copy in halos[1]:
                    copy.wait_recv()
            build_rim(section + 1, dims, halo_ref, corner_ref, plane_ref.at[section + 1])
            for copy in carried[section]:
                copy.wait_recv()
            low = section * moving
            rows_ref[count + low : count + low + moving, :] = arrived_ref[low : low + moving, :]
            carried.append(send_rows(section + 1))

    for copy in carried[sections - 1]:
        copy.wait_recv()
    for copy in heads[sections - 1]:
        copy.wait_recv()
    place_arrivals(sections - 1, arrivals(sections - 1), inverse_ref, head_ref)
    for copies in halos + carried + heads:
        for copy in copies:
            copy.wait_send()


def place_arrivals(section, came, inverse_ref, head_ref):
    for b in range(head_ref.shape[1] // LANES):
        span = slice(b * LANES, (b + 1) * LANES)
        where_ = spread_row(inverse_ref[section, b : b + 1, :])
        head_ref[:, span] = select_lanes(came, where_, head_ref[:, span])


def last_kernel(cap, rows_ref, arrived_ref, head_ref, index_ref, out_ref, final_ref):
    count, width = out_ref.shape
    sections = index_ref.shape[0]
    moving = 8 * cap
    chunks = moving // LANES
    final_ref[0:count, :] = rows_ref[0:count, :]
    for section in range(sections):

        def body(row, carry):
            first = section * moving + row * LANES
            for u in range(LANES):
                goal = index_ref[section, chunks + row, u]
                final_ref[pl.ds(goal, 1), :] = arrived_ref[pl.ds(first + (u ^ cap), 1), :]
            return carry

        lax.fori_loop(0, chunks, body, 0)
    lanes = lax.broadcasted_iota(jnp.int32, (LANES, width), 1)
    for b in range(count // LANES):
        span = slice(b * LANES, (b + 1) * LANES)
        full = jnp.concatenate([head_ref[:, span], jnp.zeros((width - 8, LANES), jnp.float32)], axis=0)
        out_ref[span, :] = jnp.where(lanes < 6, full.T, final_ref[span, :])


def local(sizes, cap, state, velocity, cells, slots, counts):
    sections, _, cx, cy, depth = velocity.shape
    count, width = state.shape
    moving = 8 * cap
    chunks = moving // LANES
    fields = sections * 3
    field = velocity.reshape(fields, cx, cy, depth)
    inner = cx * cy
    rim = 2 * cx + 2 * cy
    rows, arrived, head, index, _ = pl.pallas_call(
        functools.partial(steps_kernel, sizes, cap),
        out_shape=(
            pltpu.VMEM((count + (sections - 1) * moving, width), jnp.float32),
            pltpu.VMEM((sections * moving, width), jnp.float32),
            pltpu.VMEM((8, count), jnp.float32),
            pltpu.SMEM((sections, 2 * chunks, LANES), jnp.int32),
            pltpu.SMEM(counts.shape, jnp.int32),
        ),
        in_specs=[ANY] * 5,
        out_specs=(VMEM, VMEM, VMEM, SMEM, SMEM),
        scratch_shapes=[
            pltpu.VMEM(field.shape, field.dtype),
            pltpu.VMEM(cells.shape, jnp.int32),
            pltpu.VMEM(slots.shape, jnp.int32),
            pltpu.VMEM((sections, 2 * chunks, LANES), jnp.int32),
            pltpu.VMEM((sections, count // LANES, LANES), jnp.int32),
            pltpu.VMEM((sections, chunks, LANES), jnp.int32),
            pltpu.VMEM((chunks, 8, LANES), jnp.int32),
            pltpu.VMEM((chunks, 8, LANES), jnp.float32),
            pltpu.VMEM((sections, moving, width), jnp.float32),
            pltpu.VMEM((sections, 3 * depth, inner + 2 * LANES), jnp.bfloat16),
            pltpu.VMEM((2, fields, cx, depth), field.dtype),
            pltpu.VMEM((2, 4, 8, depth), jnp.float32),
            pltpu.VMEM((fields, rim, depth), field.dtype),
            pltpu.VMEM((2, 4, 8, depth), jnp.float32),
            pltpu.VMEM((sections, chunks, 8, LANES), jnp.float32),
            pltpu.VMEM((sections, 8, 8, LANES), jnp.float32),
            pltpu.SemaphoreType.DMA((6 + sections,)),
            pltpu.SemaphoreType.DMA((2 + 2 * sections, 8)),
            pltpu.SemaphoreType.DMA((2 + 2 * sections, 8)),
        ],
        compiler_params=pltpu.CompilerParams(collective_id=0, has_side_effects=True),
    )(state, field, cells, slots, counts)
    rows, arrived, head = (pltpu.with_memory_space_constraint(x, pltpu.VMEM) for x in (rows, arrived, head))
    index = pltpu.with_memory_space_constraint(index, pltpu.SMEM)
    return pl.pallas_call(
        functools.partial(last_kernel, cap),
        out_shape=jax.ShapeDtypeStruct((count, width), jnp.float32),
        in_specs=[VMEM, VMEM, VMEM, SMEM],
        out_specs=VMEM,
        scratch_shapes=[pltpu.VMEM((count + SPARE, width), jnp.float32)],
    )(rows, arrived, head, index)


def solution(mesh):
    return jax.shard_map(
        functools.partial(local, (mesh.shape["gx"], mesh.shape["gy"]), 64),
        mesh=mesh,
        in_specs=(
            P(("gx", "gy"), None),
            P(None, None, "gx", "gy", None),
            P(None, None, ("gx", "gy")),
            P(None, ("gx", "gy")),
            P(None, "gx", "gy", None),
        ),
        out_specs=P(("gx", "gy"), None),
        check_vma=False,
    )
```

```python
import functools

import jax
import jax.numpy as jnp
from jax import lax
from jax.experimental import pallas as pl
from jax.experimental.pallas import tpu as pltpu
from jax.sharding import PartitionSpec as P

GAMMA = (8.0 / 15.0, 5.0 / 12.0, 3.0 / 4.0)
ZETA = (0.0, -17.0 / 60.0, -5.0 / 12.0)
OFFSETS = ((1, 0), (-1, 0), (0, 1), (0, -1), (1, 1), (-1, -1), (1, -1), (-1, 1))
LANES = 128
SPARE = 8
TOP = 65535.0
BLOCK = 512
MESH = pl.DeviceIdType.MESH
VMEM = pl.BlockSpec(memory_space=pltpu.VMEM)
SMEM = pl.BlockSpec(memory_space=pltpu.SMEM)
ANY = pl.BlockSpec(memory_space=pl.ANY)


def neighbour(r, sizes):
    off_x, off_y = OFFSETS[r]
    i, j = lax.axis_index("gx"), lax.axis_index("gy")
    return (lax.rem(i + off_x + sizes[0], sizes[0]), lax.rem(j + off_y + sizes[1], sizes[1]))


def send(r, src, dst, sems, group, sizes):
    pltpu.make_async_remote_copy(
        src_ref=src,
        dst_ref=dst,
        send_sem=sems[0].at[group],
        recv_sem=sems[1].at[group],
        device_id=neighbour(r, sizes),
        device_id_type=MESH,
    ).start()


def whole(everything, sems, group, sizes):
    return pltpu.make_async_remote_copy(
        src_ref=everything,
        dst_ref=everything,
        send_sem=sems[0].at[group],
        recv_sem=sems[1].at[group],
        device_id=neighbour(0, sizes),
        device_id_type=MESH,
    )


def tile(x, k):
    return x[:, k * LANES : (k + 1) * LANES]


def spread_row(row):
    return jnp.broadcast_to(row, (8, LANES))


def select_lanes(tiles, where_, start):
    low, high = where_ & (LANES - 1), where_ >> 7
    out = start
    for k, source in enumerate(tiles):
        out = jnp.where(high == k, jnp.take_along_axis(source, low, axis=1), out)
    return out


def look_up(table, where_):
    low, high = spread_row(where_ & (LANES - 1)), spread_row(where_ >> 7)
    row = lax.broadcasted_iota(jnp.int32, (8, LANES), 0)
    best = jnp.zeros((8, LANES), jnp.int32)
    for g in range(table.shape[0] // 8):
        got = jnp.take_along_axis(table[8 * g : 8 * g + 8], low, axis=1)
        best = jnp.where(row + 8 * g == high, got, best)
    return jnp.max(best, axis=0, keepdims=True)


def cell_weights(size, cell, frac):
    spots = lax.broadcasted_iota(jnp.int32, (size, cell.shape[1]), 0)
    low, high = 1.0 - frac, frac
    inside = jnp.where(spots == cell, low, jnp.where(spots == cell + 1, high, 0.0))
    return inside, jnp.where(cell == -1, low, 0.0), jnp.where(cell == size - 1, high, 0.0)


def halves(value):
    high = value.astype(jnp.bfloat16)
    return high, (value - high.astype(jnp.float32)).astype(jnp.bfloat16)


def sample(section, dims, head, cell, plane_ref):
    cx, cy = dims
    inner = cx * cy
    depth = plane_ref.shape[0] // 3
    block = head.shape[1]
    wx, wx_low, wx_high = cell_weights(cx, cell[0:1], head[0:1])
    wy, wy_low, wy_high = cell_weights(cy, cell[1:2], head[1:2])
    wz, _, _ = cell_weights(depth, cell[2:3], head[2:3])
    own = jnp.concatenate([wx[x : x + 1] * wy for x in range(cx)], axis=0)
    rim = [wx_high * wy, wx_low * wy, wx * wy_high, wx * wy_low]
    rim += [wx_high * wy_high, wx_low * wy_low, wx_high * wy_low, wx_low * wy_high]
    rim += [jnp.zeros((LANES - 2 * cx - 2 * cy - 4, block), jnp.float32)]
    own_high, own_low = halves(own)
    rim = jnp.concatenate(halves(jnp.concatenate(rim, axis=0)), axis=0)
    inside = plane_ref[:, 0:inner]
    columns = jnp.dot(inside, own_high, preferred_element_type=jnp.float32)
    columns = columns + jnp.dot(inside, own_low, preferred_element_type=jnp.float32)
    columns = columns + jnp.dot(plane_ref[:, inner:], rim, preferred_element_type=jnp.float32)
    speed = jnp.concatenate(
        [jnp.sum(columns[k * depth : (k + 1) * depth] * wz, axis=0, keepdims=True) for k in range(3)],
        axis=0,
    )
    moved = head[0:3] + GAMMA[section] * speed + ZETA[section] * head[3:6]
    return jnp.concatenate([moved, speed, jnp.ones((2, block), jnp.float32)], axis=0)


def sample_all(section, dims, cells_ref, head_ref, plane_ref):
    block = BLOCK

    def body(step, carry):
        span = pl.ds(pl.multiple_of(step * block, block), block)
        head_ref[:, span] = sample(section, dims, head_ref[:, span], cells_ref[section, :, span], plane_ref)
        return carry

    lax.fori_loop(0, head_ref.shape[1] // block, body, 0)


def gather_rows(index_ref, source_ref, target_ref):
    def body(row, carry):
        for u in range(LANES):
            target_ref[pl.ds(row * LANES + u, 1), :] = source_ref[pl.ds(index_ref[row, u], 1), :]
        return carry

    lax.fori_loop(0, target_ref.shape[0] // LANES, body, 0)


def encode(rows):
    lane = lax.broadcasted_iota(jnp.int32, rows.shape, 1)
    top = jnp.max(jnp.where(lane < 6, 0.0, rows), axis=1, keepdims=True)
    power = jnp.clip(jnp.floor(-jnp.log2(top)), 0.0, 100.0)
    code = jnp.minimum(rows * (jnp.exp2(power) * TOP) + 0.5, TOP)
    return jnp.where(lane < 6, power, code).astype(jnp.int32)


def decode(code):
    value = code.astype(jnp.float32)
    return value * (jnp.exp2(-value[:, 0:1]) * (1.0 / TOP))


def encode_rows(leave_ref, packed_ref):
    half = packed_ref.shape[0] // 8
    for r in range(8):
        first = encode(leave_ref[2 * half * r : 2 * half * r + half, :])
        second = encode(leave_ref[2 * half * r + half : 2 * half * (r + 1), :])
        packed_ref[half * r : half * (r + 1), :] = (first << 16) | second


def decode_rows(packed_ref, target_ref, start):
    half = packed_ref.shape[0] // 8
    for r in range(8):
        word = packed_ref[half * r : half * (r + 1), :]
        low = start + 2 * half * r
        target_ref[low : low + half, :] = decode((word >> 16) & 65535)
        target_ref[low + half : low + 2 * half, :] = decode(word & 65535)


def find_edges(fields, dims, v_ref, yface_ref, away_ref):
    cx, cy = dims
    inner = cx * cy
    row = lax.broadcasted_iota(jnp.int32, (2 * cx + 8, inner), 0)
    place = lax.broadcasted_iota(jnp.int32, (2 * cx + 8, inner), 1)
    want = jnp.where(row < cx, row * cy + cy - 1, (row - cx) * cy)
    for d, spot in enumerate((inner - 1, 0, (cx - 1) * cy, cy - 1)):
        want = jnp.where(row == 2 * cx + d, spot, want)
    pick = jnp.where(want == place, 1.0, 0.0).astype(jnp.bfloat16)
    for f in fields:
        edge = jnp.dot(pick, v_ref[f].reshape(inner, v_ref.shape[3]), preferred_element_type=jnp.float32)
        yface_ref[0, f] = edge[0:cx].astype(jnp.bfloat16)
        yface_ref[1, f] = edge[cx : 2 * cx].astype(jnp.bfloat16)
        group, line = (0, f) if f < 3 else (1, f - 3)
        for d in range(4):
            away_ref[group, d, line : line + 1, :] = edge[2 * cx + d : 2 * cx + d + 1]


def build_inside(section, dims, v_ref, plane_ref):
    inner = dims[0] * dims[1]
    depth = v_ref.shape[3]
    for k in range(3):
        own = v_ref[3 * section + k].reshape(inner, depth)
        plane_ref[pl.ds(k * depth, depth), 0:inner] = own.T


def build_rim(section, dims, halo_ref, corner_ref, plane_ref):
    inner = dims[0] * dims[1]
    depth = halo_ref.shape[2]
    for k in range(3):
        f = 3 * section + k
        group, line = (0, f) if f < 3 else (1, f - 3)
        faces = halo_ref[f].astype(jnp.float32)
        corners = [corner_ref[group, d, line : line + 1, :] for d in range(4)]
        filler = jnp.zeros((LANES - faces.shape[0] - 4, depth), jnp.float32)
        edge = jnp.concatenate([faces] + corners + [filler], axis=0).T.astype(jnp.bfloat16)
        plane_ref[pl.ds(k * depth, depth), inner : inner + LANES] = edge
        plane_ref[pl.ds(k * depth, depth), inner + LANES :] = edge


def plan(section, cap, count, slots_ref, counts_ref):
    moving = 8 * cap
    blocks = count // LANES
    slot = slots_ref[section : section + 1, 0:moving]
    lanes = lax.broadcasted_iota(jnp.int32, (1, moving), 1)
    limit = jnp.zeros((1, moving), jnp.int32)
    for r in range(8):
        limit = jnp.where(lanes >= r * cap, counts_ref[section, 0, 0, r], limit)
    taken = lax.rem(lanes, cap) < limit
    goal = jnp.where(taken, slot, count)
    value = jnp.where(taken, (lanes ^ cap) + 1, 0)
    low, high = slot & (LANES - 1), slot >> 7
    line = lax.broadcasted_iota(jnp.int32, (blocks, moving), 0)
    upper = jnp.where(line == high, (value >> 5).astype(jnp.float32), 0.0)
    lower = jnp.where(line == high, (value & 31).astype(jnp.float32), 0.0)
    left = jnp.concatenate([upper, lower], axis=0).astype(jnp.bfloat16)
    spots = lax.broadcasted_iota(jnp.int32, (LANES, moving), 0)
    right = jnp.where(spots == low, 1.0, 0.0).astype(jnp.bfloat16)
    both = lax.dot_general(left, right, (((1,), (1,)), ((), ())), preferred_element_type=jnp.float32)
    inverse = (both[0:blocks] * 32.0 + both[blocks:]).astype(jnp.int32)
    return slot, goal, inverse


def steps_kernel(
    sizes,
    cap,
    state_hbm,
    v_hbm,
    cells_hbm,
    slots_hbm,
    counts_hbm,
    base_ref,
    merged_ref,
    index_ref,
    counts_ref,
    places_ref,
    rows_ref,
    packed_ref,
    arrived_ref,
    head_ref,
    v_ref,
    cells_ref,
    slots_ref,
    staged_ref,
    final_ref,
    inverse_ref,
    from_ref,
    there_ref,
    own_ref,
    leave_ref,
    plane_ref,
    yface_ref,
    away_ref,
    halo_ref,
    corner_ref,
    head_out_ref,
    head_in_ref,
    local_sem,
    send_sem,
    recv_sem,
):
    sems = (send_sem, recv_sem)
    sections, _, count = cells_ref.shape
    cx, cy = v_ref.shape[1], v_ref.shape[2]
    dims = (cx, cy)
    moving = 8 * cap
    chunks = moving // LANES
    blocks = count // LANES
    fields = 3 * sections
    starts = (0, cy, 2 * cy, 2 * cy + cx)
    widths = (cy, cy, cx, cx)

    barrier = pltpu.get_barrier_semaphore()
    for r in range(8):
        pl.semaphore_signal(barrier, inc=1, device_id=neighbour(r, sizes), device_id_type=MESH)

    def fetch(k, src, dst):
        copy = pltpu.make_async_copy(src, dst, local_sem.at[k])
        copy.start()
        return copy

    load_first = fetch(0, v_hbm.at[pl.ds(0, 3)], v_ref.at[pl.ds(0, 3)])
    load_slots = fetch(1, slots_hbm, slots_ref)
    load_counts = fetch(2, counts_hbm, counts_ref)
    load_state = fetch(3, state_hbm, rows_ref.at[pl.ds(0, count)])
    load_cells = fetch(4, cells_hbm, cells_ref)
    load_rest = fetch(5, v_hbm.at[pl.ds(3, fields - 3)], v_ref.at[pl.ds(3, fields - 3)])

    spans = (pl.ds(0, 3), pl.ds(3, fields - 3))

    def send_halo(group):
        span = spans[group]
        for r in range(8):
            if r < 4:
                off_x, off_y = OFFSETS[r]
                src = v_ref.at[span, cx - 1 if off_x > 0 else 0] if off_x else yface_ref.at[r - 2, span]
                dst = halo_ref.at[span, pl.ds(starts[r ^ 1], widths[r ^ 1]), :]
                send(r, src, dst, sems, 2 * group, sizes)
            else:
                src, dst = away_ref.at[group, r - 4], corner_ref.at[group, (r ^ 1) - 4]
                send(r, src, dst, sems, 2 * group + 1, sizes)
        faces = whole(halo_ref.at[span], sems, 2 * group, sizes)
        corners = whole(corner_ref.at[group], sems, 2 * group + 1, sizes)
        return [faces, corners]

    load_first.wait()
    find_edges(range(3), dims, v_ref, yface_ref, away_ref)
    pl.semaphore_wait(barrier, 8)
    halos = [send_halo(0)]

    load_slots.wait()
    load_counts.wait()
    slots, inverses = [], []
    table = lax.broadcasted_iota(jnp.int32, (blocks, LANES), 0) * LANES
    table = table + lax.broadcasted_iota(jnp.int32, (blocks, LANES), 1)
    places = []
    for section in range(sections):
        slot, goal, inverse = plan(section, cap, count, slots_ref, counts_ref)
        if section:
            packed = table * 1024 + inverses[-1]
            found = [look_up(packed, tile(slot, c)) for c in range(chunks)]
            for c in range(chunks):
                staged_ref[section, c : c + 1, :] = jnp.clip(found[c] >> 10, 0, count + section * moving - 1)
                from_ref[section, c : c + 1, :] = (found[c] & 1023) - 1
        else:
            for c in range(chunks):
                staged_ref[section, c : c + 1, :] = tile(slot, c)
        for c in range(chunks):
            staged_ref[section, chunks + c : chunks + c + 1, :] = tile(goal, c)
        places.append(fetch(6 + section, staged_ref.at[section], index_ref.at[section]))
        if section + 1 == sections:
            final_ref[...] = jnp.clip(table, 0, count + section * moving - 1)
            places.append(fetch(6 + sections, final_ref, places_ref))
        table = jnp.where(inverse > 0, inverse + (count + section * moving - 1), table)
        inverse_ref[section] = inverse - 1
        slots.append(slot)
        inverses.append(inverse)

    load_rest.wait()
    find_edges(range(3, fields), dims, v_ref, yface_ref, away_ref)
    halos.append(send_halo(1))

    def send_rows(section):
        places[section].wait()
        gather_rows(index_ref.at[section], rows_ref, leave_ref)
        encode_rows(leave_ref, packed_ref.at[section])
        half = cap // 2
        for r in range(8):
            span = pl.ds(r * half, half)
            send(r, packed_ref.at[section, span], arrived_ref.at[section, span], sems, 4 + section, sizes)
        return [whole(arrived_ref.at[section], sems, 4 + section, sizes)]

    load_state.wait()
    carried = [send_rows(0)]
    build_inside(0, dims, v_ref, plane_ref.at[0])
    for b in range(blocks):
        head_ref[:, b * LANES : (b + 1) * LANES] = rows_ref[b * LANES : (b + 1) * LANES, :].T[0:8]

    load_cells.wait()
    line = lax.broadcasted_iota(jnp.int32, (8, LANES), 0)
    packed = []
    for b in range(blocks):
        span = slice(b * LANES, (b + 1) * LANES)
        both = jnp.zeros((8, LANES), jnp.int32)
        for section in range(sections):
            spot = cells_ref[section, :, span]
            word = (spot[0:1] + 1) + (spot[1:2] + 1) * 1024 + spot[2:3] * 1048576
            both = jnp.where(line == section, spread_row(word), both)
        packed.append(both)
    for c in range(chunks):
        where_ = spread_row(tile(slots[0], c))
        for section in range(1, sections):
            where_ = jnp.where(line == section, spread_row(tile(slots[section], c)), where_)
        there_ref[c] = select_lanes(packed, where_, jnp.zeros((8, LANES), jnp.int32))

    def pick_own(section):
        tiles = [head_ref[:, b * LANES : (b + 1) * LANES] for b in range(blocks)]
        for c in range(chunks):
            where_ = spread_row(slots_ref[section : section + 1, c * LANES : (c + 1) * LANES])
            own_ref[c] = select_lanes(tiles, where_, jnp.zeros((8, LANES), jnp.float32))

    def arrivals(section):
        first = lax.broadcasted_iota(jnp.int32, (8, LANES), 1) < cap
        return [
            jnp.where(first, head_in_ref[section, 2 * c], head_in_ref[section, 2 * c + 1]) for c in range(chunks)
        ]

    pick_own(0)
    heads = []
    for section in range(sections):
        if section == 0:
            for copy in halos[0]:
                copy.wait_recv()
            build_rim(0, dims, halo_ref, corner_ref, plane_ref.at[0])
            leaving = [own_ref[c] for c in range(chunks)]
        else:
            for copy in heads[section - 1]:
                copy.wait_recv()
            came = arrivals(section - 1)
            leaving = [
                select_lanes(came, spread_row(from_ref[section, c : c + 1, :]), own_ref[c]) for c in range(chunks)
            ]
        word = jnp.concatenate([there_ref[c, section : section + 1, :] for c in range(chunks)], axis=1)
        spot = jnp.concatenate([(word & 1023) - 1, ((word >> 10) & 1023) - 1, word >> 20], axis=0)
        leaving = sample(section, dims, jnp.concatenate(leaving, axis=1), spot, plane_ref.at[section])
        for c in range(chunks):
            head_out_ref[section, c] = tile(leaving, c)
        group = 4 + sections + section
        for r in range(8):
            send(r, head_out_ref.at[section, r // 2], head_in_ref.at[section, r], sems, group, sizes)
        heads.append([whole(head_in_ref.at[section], sems, group, sizes)])

        if section:
            place_arrivals(section - 1, arrivals(section - 1), inverse_ref, head_ref)
        sample_all(section, dims, cells_ref, head_ref, plane_ref.at[section])
        if section + 1 < sections:
            pick_own(section + 1)
            build_inside(section + 1, dims, v_ref, plane_ref.at[section + 1])
            if section == 0:
                for copy in halos[1]:
                    copy.wait_recv()
            build_rim(section + 1, dims, halo_ref, corner_ref, plane_ref.at[section + 1])
            for copy in carried[section]:
                copy.wait_recv()
            decode_rows(arrived_ref.at[section], rows_ref, count + section * moving)
            carried.append(send_rows(section + 1))

    places[sections].wait()
    gather_rows(places_ref, rows_ref, base_ref)
    for b in range(blocks):
        span = slice(b * LANES, (b + 1) * LANES)
        base_ref[span, :] = merge_head(head_ref[:, span], base_ref[span, :])
    for copy in carried[sections - 1]:
        copy.wait_recv()
    decode_rows(arrived_ref.at[sections - 1], merged_ref, 0)
    for copies in halos + carried + heads[:-1]:
        for copy in copies:
            copy.wait_send()
    for copy in heads[sections - 1]:
        copy.wait_recv()
    for c, came in enumerate(arrivals(sections - 1)):
        span = slice(c * LANES, (c + 1) * LANES)
        merged_ref[span, :] = merge_head(came, merged_ref[span, :])
    for copy in heads[sections - 1]:
        copy.wait_send()


def merge_head(head, rows):
    lane = lax.broadcasted_iota(jnp.int32, rows.shape, 1)
    full = jnp.concatenate([head, jnp.zeros((rows.shape[1] - 8, LANES), jnp.float32)], axis=0)
    return jnp.where(lane < 6, full.T, rows)


def place_arrivals(section, came, inverse_ref, head_ref):
    for b in range(head_ref.shape[1] // LANES):
        span = slice(b * LANES, (b + 1) * LANES)
        where_ = spread_row(inverse_ref[section, b : b + 1, :])
        head_ref[:, span] = select_lanes(came, where_, head_ref[:, span])


def last_kernel(cap, base_ref, merged_ref, index_ref, out_hbm, final_ref, sem):
    count = out_hbm.shape[0]
    last = index_ref.shape[0] - 1
    chunks = 8 * cap // LANES
    final_ref[0:count, :] = base_ref[...]

    def body(row, carry):
        for u in range(LANES):
            goal = index_ref[last, chunks + row, u]
            final_ref[pl.ds(goal, 1), :] = merged_ref[pl.ds(row * LANES + (u ^ cap), 1), :]
        return carry

    lax.fori_loop(0, chunks, body, 0)
    copy = pltpu.make_async_copy(final_ref.at[pl.ds(0, count)], out_hbm, sem)
    copy.start()
    copy.wait()


def local(sizes, cap, state, velocity, cells, slots, counts):
    sections, _, cx, cy, depth = velocity.shape
    count, width = state.shape
    moving = 8 * cap
    chunks = moving // LANES
    fields = sections * 3
    field = velocity.reshape(fields, cx, cy, depth)
    inner = cx * cy
    rim = 2 * cx + 2 * cy
    half = moving // 2
    base, merged, index, _, _ = pl.pallas_call(
        functools.partial(steps_kernel, sizes, cap),
        out_shape=(
            pltpu.VMEM((count, width), jnp.float32),
            pltpu.VMEM((moving, width), jnp.float32),
            pltpu.SMEM((sections, 2 * chunks, LANES), jnp.int32),
            pltpu.SMEM(counts.shape, jnp.int32),
            pltpu.SMEM((count // LANES, LANES), jnp.int32),
        ),
        in_specs=[ANY] * 5,
        out_specs=(VMEM, VMEM, SMEM, SMEM, SMEM),
        scratch_shapes=[
            pltpu.VMEM((count + (sections - 1) * moving, width), jnp.float32),
            pltpu.VMEM((sections, half, width), jnp.int32),
            pltpu.VMEM((sections, half, width), jnp.int32),
            pltpu.VMEM((8, count), jnp.float32),
            pltpu.VMEM(field.shape, field.dtype),
            pltpu.VMEM(cells.shape, jnp.int32),
            pltpu.VMEM(slots.shape, jnp.int32),
            pltpu.VMEM((sections, 2 * chunks, LANES), jnp.int32),
            pltpu.VMEM((count // LANES, LANES), jnp.int32),
            pltpu.VMEM((sections, count // LANES, LANES), jnp.int32),
            pltpu.VMEM((sections, chunks, LANES), jnp.int32),
            pltpu.VMEM((chunks, 8, LANES), jnp.int32),
            pltpu.VMEM((chunks, 8, LANES), jnp.float32),
            pltpu.VMEM((moving, width), jnp.float32),
            pltpu.VMEM((sections, 3 * depth, inner + 2 * LANES), jnp.bfloat16),
            pltpu.VMEM((2, fields, cx, depth), field.dtype),
            pltpu.VMEM((2, 4, 8, depth), jnp.float32),
            pltpu.VMEM((fields, rim, depth), field.dtype),
            pltpu.VMEM((2, 4, 8, depth), jnp.float32),
            pltpu.VMEM((sections, chunks, 8, LANES), jnp.float32),
            pltpu.VMEM((sections, 8, 8, LANES), jnp.float32),
            pltpu.SemaphoreType.DMA((7 + sections,)),
            pltpu.SemaphoreType.DMA((4 + 2 * sections,)),
            pltpu.SemaphoreType.DMA((4 + 2 * sections,)),
        ],
        compiler_params=pltpu.CompilerParams(collective_id=0, has_side_effects=True),
    )(state, field, cells, slots, counts)
    base, merged = (pltpu.with_memory_space_constraint(x, pltpu.VMEM) for x in (base, merged))
    index = pltpu.with_memory_space_constraint(index, pltpu.SMEM)
    return pl.pallas_call(
        functools.partial(last_kernel, cap),
        out_shape=jax.ShapeDtypeStruct((count, width), jnp.float32),
        in_specs=[VMEM, VMEM, SMEM],
        out_specs=ANY,
        scratch_shapes=[pltpu.VMEM((count + SPARE, width), jnp.float32), pltpu.SemaphoreType.DMA],
    )(base, merged, index)


def solution(mesh):
    return jax.shard_map(
        functools.partial(local, (mesh.shape["gx"], mesh.shape["gy"]), 64),
        mesh=mesh,
        in_specs=(
            P(("gx", "gy"), None),
            P(None, None, "gx", "gy", None),
            P(None, None, ("gx", "gy")),
            P(None, ("gx", "gy")),
            P(None, "gx", "gy", None),
        ),
        out_specs=P(("gx", "gy"), None),
        check_vma=False,
    )
```

```python
import functools

import jax
import jax.numpy as jnp
from jax import lax
from jax.experimental import pallas as pl
from jax.experimental.pallas import tpu as pltpu
from jax.sharding import PartitionSpec as P

GAMMA = (8.0 / 15.0, 5.0 / 12.0, 3.0 / 4.0)
ZETA = (0.0, -17.0 / 60.0, -5.0 / 12.0)
OFFSETS = ((1, 0), (-1, 0), (0, 1), (0, -1), (1, 1), (-1, -1), (1, -1), (-1, 1))
LANES = 128
FAR = ((0, 2), (0, -2))
CORNER_SLOT = (2, 0, 3, 1)
SPARE = 8
TOP = 65535.0
BLOCK = 512
MESH = pl.DeviceIdType.MESH
VMEM = pl.BlockSpec(memory_space=pltpu.VMEM)
SMEM = pl.BlockSpec(memory_space=pltpu.SMEM)
ANY = pl.BlockSpec(memory_space=pl.ANY)


def neighbour(offset, sizes):
    off_x, off_y = offset
    i, j = lax.axis_index("gx"), lax.axis_index("gy")
    return (lax.rem(i + off_x + sizes[0], sizes[0]), lax.rem(j + off_y + sizes[1], sizes[1]))


def send(offset, src, dst, sems, group, sizes):
    pltpu.make_async_remote_copy(
        src_ref=src,
        dst_ref=dst,
        send_sem=sems[0].at[group],
        recv_sem=sems[1].at[group],
        device_id=neighbour(offset, sizes),
        device_id_type=MESH,
    ).start()


def whole(everything, sems, group, sizes):
    return pltpu.make_async_remote_copy(
        src_ref=everything,
        dst_ref=everything,
        send_sem=sems[0].at[group],
        recv_sem=sems[1].at[group],
        device_id=neighbour(OFFSETS[0], sizes),
        device_id_type=MESH,
    )


def tile(x, k):
    return x[:, k * LANES : (k + 1) * LANES]


def spread_row(row):
    return jnp.broadcast_to(row, (8, LANES))


def select_lanes(tiles, where_, start):
    low, high = where_ & (LANES - 1), where_ >> 7
    out = start
    for k, source in enumerate(tiles):
        out = jnp.where(high == k, jnp.take_along_axis(source, low, axis=1), out)
    return out


def look_up(table, where_):
    low, high = spread_row(where_ & (LANES - 1)), spread_row(where_ >> 7)
    row = lax.broadcasted_iota(jnp.int32, (8, LANES), 0)
    best = jnp.zeros((8, LANES), jnp.int32)
    for g in range(table.shape[0] // 8):
        got = jnp.take_along_axis(table[8 * g : 8 * g + 8], low, axis=1)
        best = jnp.where(row + 8 * g == high, got, best)
    return jnp.max(best, axis=0, keepdims=True)


def cell_weights(size, cell, frac):
    spots = lax.broadcasted_iota(jnp.int32, (size, cell.shape[1]), 0)
    low, high = 1.0 - frac, frac
    inside = jnp.where(spots == cell, low, jnp.where(spots == cell + 1, high, 0.0))
    return inside, jnp.where(cell == -1, low, 0.0), jnp.where(cell == size - 1, high, 0.0)


def halves(value):
    high = value.astype(jnp.bfloat16)
    return high, (value - high.astype(jnp.float32)).astype(jnp.bfloat16)


def sum_depth(columns, wz):
    depth = wz.shape[0]
    return jnp.concatenate(
        [jnp.sum(columns[k * depth : (k + 1) * depth] * wz, axis=0, keepdims=True) for k in range(3)],
        axis=0,
    )


def multiply(plane, parts):
    total = jnp.dot(plane, parts[0], preferred_element_type=jnp.float32)
    for part in parts[1:]:
        total = total + jnp.dot(plane, part, preferred_element_type=jnp.float32)
    return total


def own_weights(wx, wy):
    return jnp.concatenate([wx[x : x + 1] * wy for x in range(wx.shape[0])], axis=0)


def rim_weights(wxs, wys):
    wx, wx_low, wx_high = wxs
    wy, wy_low, wy_high = wys
    rim = [wx_high * wy, wx_low * wy, wx * wy_high, wx * wy_low]
    rim += [wx_high * wy_high, wx_low * wy_low, wx_high * wy_low, wx_low * wy_high]
    filled = sum(part.shape[0] for part in rim)
    rim += [jnp.zeros((LANES - filled, wy.shape[1]), jnp.float32)]
    return jnp.concatenate(halves(jnp.concatenate(rim, axis=0)), axis=0)


def weights_of(dims, depth, head, cell):
    wxs = cell_weights(dims[0], cell[0:1], head[0:1])
    wys = cell_weights(dims[1], cell[1:2], head[1:2])
    wz, _, _ = cell_weights(depth, cell[2:3], head[2:3])
    return wxs, wys, wz


def advance(section, head, speed):
    moved = head[0:3] + GAMMA[section] * speed + ZETA[section] * head[3:6]
    return jnp.concatenate([moved, speed, jnp.ones((2, speed.shape[1]), jnp.float32)], axis=0)


def sample(section, dims, head, cell, plane_ref):
    inner = dims[0] * dims[1]
    wxs, wys, wz = weights_of(dims, plane_ref.shape[0] // 3, head, cell)
    columns = multiply(plane_ref[:, 0:inner], halves(own_weights(wxs[0], wys[0])))
    columns = columns + multiply(plane_ref[:, inner:], [rim_weights(wxs, wys)])
    return advance(section, head, sum_depth(columns, wz))


def unpack_cell(word):
    return jnp.concatenate([(word & 63) - 1, ((word >> 6) & 63) - 1, word >> 12], axis=0)


def sample_all(section, dims, cells_ref, head_ref, plane_ref):
    block = BLOCK

    for step in range(head_ref.shape[1] // block):
        span = slice(step * block, (step + 1) * block)
        head_ref[:, span] = sample(section, dims, head_ref[:, span], cells_ref[section, :, span], plane_ref)


def gather_rows(index_ref, source_ref, target_ref):
    def body(row, carry):
        for u in range(LANES):
            target_ref[pl.ds(row * LANES + u, 1), :] = source_ref[pl.ds(index_ref[row, u], 1), :]
        return carry

    lax.fori_loop(0, target_ref.shape[0] // LANES, body, 0)


def encode(rows):
    lane = lax.broadcasted_iota(jnp.int32, rows.shape, 1)
    top = jnp.max(jnp.where(lane < 6, 0.0, rows), axis=1, keepdims=True)
    power = jnp.clip(jnp.floor(-jnp.log2(top)), 0.0, 100.0)
    code = jnp.minimum(rows * (jnp.exp2(power) * TOP) + 0.5, TOP)
    return jnp.where(lane < 6, power, code).astype(jnp.int32)


def decode(code):
    value = code.astype(jnp.float32)
    return value * (jnp.exp2(-value[:, 0:1]) * (1.0 / TOP))


def encode_rows(leave_ref, packed_ref):
    half = packed_ref.shape[0] // 8
    for r in range(8):
        first = encode(leave_ref[2 * half * r : 2 * half * r + half, :])
        second = encode(leave_ref[2 * half * r + half : 2 * half * (r + 1), :])
        packed_ref[half * r : half * (r + 1), :] = (first << 16) | second


def decode_rows(packed_ref, target_ref, start):
    half = packed_ref.shape[0] // 8
    for r in range(8):
        word = packed_ref[half * r : half * (r + 1), :]
        low = start + 2 * half * r
        target_ref[low : low + half, :] = decode((word >> 16) & 65535)
        target_ref[low + half : low + 2 * half, :] = decode(word & 65535)


def find_edges(fields, dims, v_ref, yface_ref, away_ref):
    cx, cy = dims
    inner = cx * cy
    row = lax.broadcasted_iota(jnp.int32, (2 * cx + 8, inner), 0)
    place = lax.broadcasted_iota(jnp.int32, (2 * cx + 8, inner), 1)
    want = jnp.where(row < cx, row * cy + cy - 1, (row - cx) * cy)
    for d, spot in enumerate((inner - 1, 0, (cx - 1) * cy, cy - 1)):
        want = jnp.where(row == 2 * cx + d, spot, want)
    pick = jnp.where(want == place, 1.0, 0.0).astype(jnp.bfloat16)
    for f in fields:
        edge = jnp.dot(pick, v_ref[f].reshape(inner, v_ref.shape[3]), preferred_element_type=jnp.float32)
        yface_ref[0, f] = edge[0:cx].astype(jnp.bfloat16)
        yface_ref[1, f] = edge[cx : 2 * cx].astype(jnp.bfloat16)
        group, line = (0, f) if f < 3 else (1, f - 3)
        for d in range(4):
            away_ref[group, d, line : line + 1, :] = edge[2 * cx + d : 2 * cx + d + 1]


def build_inside(section, dims, v_ref, plane_ref):
    inner = dims[0] * dims[1]
    depth = v_ref.shape[3]
    for k in range(3):
        own = v_ref[3 * section + k].reshape(inner, depth)
        plane_ref[pl.ds(k * depth, depth), 0:inner] = own.T


def build_rim(section, dims, halo_ref, corner_ref, plane_ref, with_plus=True):
    cx, cy = dims
    inner = cx * cy
    depth = halo_ref.shape[2]
    for k in range(3):
        f = 3 * section + k
        group, line = (0, f) if f < 3 else (1, f - 3)
        plus = halo_ref[f, 0:cy, :].astype(jnp.float32) if with_plus else jnp.zeros((cy, depth), jnp.float32)
        faces = [plus, halo_ref[f, cy:, :].astype(jnp.float32)]
        corners = [corner_ref[group, CORNER_SLOT[d], line : line + 1, :] for d in range(4)]
        if not with_plus:
            corners = [jnp.zeros((1, depth), jnp.float32) if d % 2 == 0 else corners[d] for d in range(4)]
        filler = jnp.zeros((LANES - 2 * cx - 2 * cy - 4, depth), jnp.float32)
        edge = jnp.concatenate(faces + corners + [filler], axis=0).T.astype(jnp.bfloat16)
        plane_ref[pl.ds(k * depth, depth), inner : inner + LANES] = edge
        plane_ref[pl.ds(k * depth, depth), inner + LANES :] = edge


def build_columns(dims, v_ref, face_ref, far_ref, column_ref):
    cx, cy = dims
    depth = v_ref.shape[3]
    for k in range(3):
        edge = []
        for side, x, above, below in ((0, 0, 1, 3), (1, cx - 1, 2, 0)):
            edge += [face_ref[1, side, k].astype(jnp.float32), v_ref[k, x].astype(jnp.float32)]
            edge += [face_ref[0, side, k].astype(jnp.float32), far_ref[0, above, k : k + 1, :]]
            edge += [jnp.zeros((LANES // 2 - 3 * cy - 2, depth), jnp.float32), far_ref[1, below, k : k + 1, :]]
        edge = jnp.concatenate(edge, axis=0).T.astype(jnp.bfloat16)
        column_ref[pl.ds(k * depth, depth), 0:LANES] = edge
        column_ref[pl.ds(k * depth, depth), LANES:] = edge


def finish_arrivals(dims, came, cap, column_ref, done_ref):
    cx, cy = dims
    half = LANES // 2
    crossed = [c for c in range(len(came)) if c != 1]
    head = jnp.concatenate([came[c] for c in crossed], axis=1)
    cell = unpack_cell(head[6:7].astype(jnp.int32))
    lanes = lax.broadcasted_iota(jnp.int32, (1, head.shape[1]), 1)
    odd = (lanes & cap) > 0
    shift = jnp.zeros((1, head.shape[1]), jnp.int32)
    for place, c in enumerate(crossed):
        for r in (2 * c, 2 * c + 1):
            here = (lanes >> 6) == 2 * place + r % 2
            shift = jnp.where(here, -cy * OFFSETS[r][1], shift)
    wx = jnp.where(odd, jnp.where(cell[0:1] == -1, 1.0 - head[0:1], 0.0), jnp.where(cell[0:1] == cx - 1, head[0:1], 0.0))
    base = jnp.where(odd, half, 0)
    first = base + ((cell[1:2] + shift + cy) & (half - 1))
    second = base + ((cell[1:2] + shift + cy + 1) & (half - 1))
    spots = lax.broadcasted_iota(jnp.int32, (LANES, head.shape[1]), 0)
    low, high = wx * (1.0 - head[1:2]), wx * head[1:2]
    weight = jnp.where(spots == first, low, jnp.where(spots == second, high, 0.0))
    wz, _, _ = cell_weights(column_ref.shape[0] // 3, cell[2:3], head[2:3])
    columns = multiply(column_ref[...], [jnp.concatenate(halves(weight), axis=0)])
    speed = head[3:6] + sum_depth(columns, wz)
    for place, c in enumerate(crossed):
        done_ref[c] = advance(0, tile(head, place), tile(speed, place))
    done_ref[1] = advance(0, came[1], came[1][3:6])


def plan(section, cap, count, slots_ref, counts_ref):
    moving = 8 * cap
    blocks = count // LANES
    slot = slots_ref[section : section + 1, 0:moving]
    lanes = lax.broadcasted_iota(jnp.int32, (1, moving), 1)
    limit = jnp.zeros((1, moving), jnp.int32)
    for r in range(8):
        limit = jnp.where(lanes >= r * cap, counts_ref[section, 0, 0, r], limit)
    taken = lax.rem(lanes, cap) < limit
    goal = jnp.where(taken, slot, count)
    value = jnp.where(taken, (lanes ^ cap) + 1, 0)
    low, high = slot & (LANES - 1), slot >> 7
    line = lax.broadcasted_iota(jnp.int32, (blocks, moving), 0)
    upper = jnp.where(line == high, (value >> 5).astype(jnp.float32), 0.0)
    lower = jnp.where(line == high, (value & 31).astype(jnp.float32), 0.0)
    left = jnp.concatenate([upper, lower], axis=0).astype(jnp.bfloat16)
    spots = lax.broadcasted_iota(jnp.int32, (LANES, moving), 0)
    right = jnp.where(spots == low, 1.0, 0.0).astype(jnp.bfloat16)
    both = lax.dot_general(left, right, (((1,), (1,)), ((), ())), preferred_element_type=jnp.float32)
    inverse = (both[0:blocks] * 32.0 + both[blocks:]).astype(jnp.int32)
    return slot, goal, inverse


def steps_kernel(
    sizes,
    cap,
    state_hbm,
    v_hbm,
    cells_hbm,
    slots_hbm,
    counts_hbm,
    base_ref,
    merged_ref,
    index_ref,
    counts_ref,
    places_ref,
    rows_ref,
    packed_ref,
    arrived_ref,
    head_ref,
    v_ref,
    cells_ref,
    slots_ref,
    staged_ref,
    final_ref,
    inverse_ref,
    from_ref,
    there_ref,
    own_ref,
    leave_ref,
    plane_ref,
    yface_ref,
    away_ref,
    halo_ref,
    corner_ref,
    face_ref,
    far_ref,
    column_ref,
    done_ref,
    late_ref,
    head_out_ref,
    head_in_ref,
    local_sem,
    send_sem,
    recv_sem,
):
    sems = (send_sem, recv_sem)
    sections, _, count = cells_ref.shape
    cx, cy = v_ref.shape[1], v_ref.shape[2]
    dims = (cx, cy)
    inner = cx * cy
    moving = 8 * cap
    chunks = moving // LANES
    blocks = count // LANES
    fields = 3 * sections
    starts = (0, cy, 2 * cy, 2 * cy + cx)
    widths = (cy, cy, cx, cx)

    barrier = pltpu.get_barrier_semaphore()
    for offset in OFFSETS + FAR:
        pl.semaphore_signal(barrier, inc=1, device_id=neighbour(offset, sizes), device_id_type=MESH)

    def fetch(k, src, dst):
        copy = pltpu.make_async_copy(src, dst, local_sem.at[k])
        copy.start()
        return copy

    load_first = fetch(0, v_hbm.at[pl.ds(0, 3)], v_ref.at[pl.ds(0, 3)])
    load_slots = fetch(1, slots_hbm, slots_ref)
    load_counts = fetch(2, counts_hbm, counts_ref)
    load_state = fetch(3, state_hbm, rows_ref.at[pl.ds(0, count)])
    load_cells = fetch(4, cells_hbm, cells_ref)
    load_rest = fetch(5, v_hbm.at[pl.ds(3, fields - 3)], v_ref.at[pl.ds(3, fields - 3)])

    spans = (pl.ds(0, 3), pl.ds(3, fields - 3))

    def send_halo(group):
        span = spans[group]
        for r in range(8):
            late = 2 if group == 0 and r in (1, 5, 7) else 0
            if r < 4:
                off_x, off_y = OFFSETS[r]
                src = v_ref.at[span, cx - 1 if off_x > 0 else 0] if off_x else yface_ref.at[r - 2, span]
                dst = halo_ref.at[span, pl.ds(starts[r ^ 1], widths[r ^ 1]), :]
                send(OFFSETS[r], src, dst, sems, 4 * group + late, sizes)
            else:
                src, dst = away_ref.at[group, r - 4], corner_ref.at[group, CORNER_SLOT[(r ^ 1) - 4]]
                send(OFFSETS[r], src, dst, sems, 4 * group + late + 1, sizes)
        if group:
            faces = whole(halo_ref.at[span], sems, 4, sizes)
            return [faces, whole(corner_ref.at[group], sems, 5, sizes)]
        early = whole(halo_ref.at[span, pl.ds(cy, 2 * cx + cy), :], sems, 0, sizes)
        late = whole(halo_ref.at[span, pl.ds(0, cy), :], sems, 2, sizes)
        corners = [whole(corner_ref.at[group, pl.ds(2 * part, 2)], sems, 2 * part + 1, sizes) for part in range(2)]
        return [early, corners[0], late, corners[1]]

    def send_columns():
        for r in (2, 3):
            for side, x in ((0, 0), (1, cx - 1)):
                send(OFFSETS[r], v_ref.at[spans[0], x], face_ref.at[(r ^ 1) - 2, side], sems, 6, sizes)
        for k, offset in enumerate(FAR):
            send(offset, away_ref.at[0], far_ref.at[1 - k], sems, 7, sizes)
        return [whole(face_ref, sems, 6, sizes), whole(far_ref, sems, 7, sizes)]

    load_first.wait()
    find_edges(range(3), dims, v_ref, yface_ref, away_ref)
    pl.semaphore_wait(barrier, len(OFFSETS + FAR))
    halos = [send_halo(0), send_columns()]

    load_slots.wait()
    load_counts.wait()
    slots, inverses = [], []
    table = lax.broadcasted_iota(jnp.int32, (blocks, LANES), 0) * LANES
    table = table + lax.broadcasted_iota(jnp.int32, (blocks, LANES), 1)
    places = []
    for section in range(sections):
        slot, goal, inverse = plan(section, cap, count, slots_ref, counts_ref)
        if section:
            packed = table * 1024 + inverses[-1]
            found = [look_up(packed, tile(slot, c)) for c in range(chunks)]
            for c in range(chunks):
                staged_ref[section, c : c + 1, :] = jnp.clip(found[c] >> 10, 0, count + section * moving - 1)
                from_ref[section, c : c + 1, :] = (found[c] & 1023) - 1
        else:
            for c in range(chunks):
                staged_ref[section, c : c + 1, :] = tile(slot, c)
        for c in range(chunks):
            staged_ref[section, chunks + c : chunks + c + 1, :] = tile(goal, c)
        places.append(fetch(6 + section, staged_ref.at[section], index_ref.at[section]))
        if section + 1 == sections:
            final_ref[...] = jnp.clip(table, 0, count + section * moving - 1)
            places.append(fetch(6 + sections, final_ref, places_ref))
        table = jnp.where(inverse > 0, inverse + (count + section * moving - 1), table)
        inverse_ref[section] = inverse - 1
        slots.append(slot)
        inverses.append(inverse)

    load_rest.wait()
    find_edges(range(3, fields), dims, v_ref, yface_ref, away_ref)
    halos.append(send_halo(1))

    def send_rows(section):
        places[section].wait()
        gather_rows(index_ref.at[section], rows_ref, leave_ref)
        encode_rows(leave_ref, packed_ref.at[section])
        half = cap // 2
        for r in range(8):
            span = pl.ds(r * half, half)
            send(OFFSETS[r], packed_ref.at[section, span], arrived_ref.at[section, span], sems, 8 + section, sizes)
        return [whole(arrived_ref.at[section], sems, 8 + section, sizes)]

    load_state.wait()
    carried = [send_rows(0)]
    for section in range(sections):
        build_inside(section, dims, v_ref, plane_ref.at[section])
    for b in range(blocks):
        head_ref[:, b * LANES : (b + 1) * LANES] = rows_ref[b * LANES : (b + 1) * LANES, :].T[0:8]

    load_cells.wait()
    line = lax.broadcasted_iota(jnp.int32, (8, LANES), 0)
    packed = []
    for b in range(blocks):
        span = slice(b * LANES, (b + 1) * LANES)
        both = jnp.zeros((8, LANES), jnp.int32)
        for section in range(sections):
            spot = cells_ref[section, :, span]
            word = (spot[0:1] + 1) + (spot[1:2] + 1) * 64 + spot[2:3] * 4096
            both = jnp.where(line == section, spread_row(word), both)
        packed.append(both)
    for c in range(chunks):
        where_ = spread_row(tile(slots[0], c))
        for section in range(1, sections):
            where_ = jnp.where(line == section, spread_row(tile(slots[section], c)), where_)
        there_ref[c] = select_lanes(packed, where_, jnp.zeros((8, LANES), jnp.int32))

    def pick_own(section):
        tiles = [head_ref[:, b * LANES : (b + 1) * LANES] for b in range(blocks)]
        for c in range(chunks):
            where_ = spread_row(slots_ref[section : section + 1, c * LANES : (c + 1) * LANES])
            own_ref[c] = select_lanes(tiles, where_, jnp.zeros((8, LANES), jnp.float32))

    def arrivals(section):
        first = lax.broadcasted_iota(jnp.int32, (8, LANES), 1) < cap
        return [
            jnp.where(first, head_in_ref[section, 2 * c], head_in_ref[section, 2 * c + 1]) for c in range(chunks)
        ]

    pick_own(0)
    heads = []
    for section in range(sections):
        group = 8 + sections + section
        word = jnp.concatenate([there_ref[c, section : section + 1, :] for c in range(chunks)], axis=1)
        cell = unpack_cell(word)
        if section == 0:
            head = jnp.concatenate([own_ref[c] for c in range(chunks)], axis=1)
            r = lax.broadcasted_iota(jnp.int32, (1, moving), 1) // cap
            plus = (r == 0) | (r == 4) | (r == 6)
            minus = (r == 1) | (r == 5) | (r == 7)
            wxs, wys, wz = weights_of(dims, v_ref.shape[3], head, cell)
            inside = plane_ref[0, :, 0:inner]
            columns = multiply(inside, halves(own_weights(wxs[0], wys[0])))
            none = jnp.zeros_like(wxs[2])
            lows = (wxs[0], jnp.where(minus, 0.0, wxs[1]), none)
            highs = (jnp.zeros_like(wxs[0]), none, jnp.where(plus, 0.0, wxs[2]))
            for copy in halos[0][0:2]:
                copy.wait_recv()
            build_rim(0, dims, halo_ref, corner_ref, plane_ref.at[0], with_plus=False)
            columns = columns + multiply(plane_ref[0, :, inner:], [rim_weights(lows, wys)])
            speed = sum_depth(columns, wz)
            tail = [word.astype(jnp.float32), jnp.ones((1, moving), jnp.float32)]
            message = jnp.concatenate([head[0:3], speed] + tail, axis=0)
            for c in range(chunks):
                head_out_ref[section, c] = tile(message, c)
            for r in (0, 4, 6):
                send(OFFSETS[r], head_out_ref.at[section, r // 2], head_in_ref.at[section, r], sems, group, sizes)
            for copy in halos[0][2:4]:
                copy.wait_recv()
            build_rim(0, dims, halo_ref, corner_ref, plane_ref.at[0])
            speed = speed + sum_depth(multiply(plane_ref[0, :, inner:], [rim_weights(highs, wys)]), wz)
            message = jnp.concatenate([head[0:3], speed] + tail, axis=0)
            for c in range(chunks):
                late_ref[c] = tile(message, c)
            for r in (1, 5, 7, 2, 3):
                send(OFFSETS[r], late_ref.at[r // 2], head_in_ref.at[section, r], sems, group, sizes)
        else:
            for copy in heads[section - 1]:
                copy.wait_recv()
            came = arrivals(section - 1)
            if section == 1:
                finish_arrivals(dims, came, cap, column_ref, done_ref)
                came = [done_ref[c] for c in range(chunks)]
            leaving = [
                select_lanes(came, spread_row(from_ref[section, c : c + 1, :]), own_ref[c]) for c in range(chunks)
            ]
            leaving = sample(section, dims, jnp.concatenate(leaving, axis=1), cell, plane_ref.at[section])
            for c in range(chunks):
                head_out_ref[section, c] = tile(leaving, c)
            for r in range(8):
                send(OFFSETS[r], head_out_ref.at[section, r // 2], head_in_ref.at[section, r], sems, group, sizes)
        heads.append([whole(head_in_ref.at[section], sems, group, sizes)])

        if section:
            came = [done_ref[c] for c in range(chunks)] if section == 1 else arrivals(section - 1)
            place_arrivals(section - 1, came, inverse_ref, head_ref)
        sample_all(section, dims, cells_ref, head_ref, plane_ref.at[section])
        if section + 1 < sections:
            pick_own(section + 1)
            if section == 0:
                for copy in halos[1] + halos[2]:
                    copy.wait_recv()
                build_columns(dims, v_ref, face_ref, far_ref, column_ref)
                for later in range(1, sections):
                    build_rim(later, dims, halo_ref, corner_ref, plane_ref.at[later])
            for copy in carried[section]:
                copy.wait_recv()
            decode_rows(arrived_ref.at[section], rows_ref, count + section * moving)
            carried.append(send_rows(section + 1))

    places[sections].wait()
    gather_rows(places_ref, rows_ref, base_ref)
    for b in range(blocks):
        span = slice(b * LANES, (b + 1) * LANES)
        base_ref[span, :] = merge_head(head_ref[:, span], base_ref[span, :])
    for copy in carried[sections - 1]:
        copy.wait_recv()
    decode_rows(arrived_ref.at[sections - 1], merged_ref, 0)
    for copies in halos + carried + heads[:-1]:
        for copy in copies:
            copy.wait_send()
    for copy in heads[sections - 1]:
        copy.wait_recv()
    for c, came in enumerate(arrivals(sections - 1)):
        span = slice(c * LANES, (c + 1) * LANES)
        merged_ref[span, :] = merge_head(came, merged_ref[span, :])
    for copy in heads[sections - 1]:
        copy.wait_send()


def merge_head(head, rows):
    lane = lax.broadcasted_iota(jnp.int32, rows.shape, 1)
    full = jnp.concatenate([head, jnp.zeros((rows.shape[1] - 8, LANES), jnp.float32)], axis=0)
    return jnp.where(lane < 6, full.T, rows)


def place_arrivals(section, came, inverse_ref, head_ref):
    for b in range(head_ref.shape[1] // LANES):
        span = slice(b * LANES, (b + 1) * LANES)
        where_ = spread_row(inverse_ref[section, b : b + 1, :])
        head_ref[:, span] = select_lanes(came, where_, head_ref[:, span])


def last_kernel(cap, base_ref, merged_ref, index_ref, out_hbm, final_ref, sem):
    count = out_hbm.shape[0]
    last = index_ref.shape[0] - 1
    chunks = 8 * cap // LANES
    final_ref[0:count, :] = base_ref[...]

    def body(row, carry):
        for u in range(LANES):
            goal = index_ref[last, chunks + row, u]
            final_ref[pl.ds(goal, 1), :] = merged_ref[pl.ds(row * LANES + (u ^ cap), 1), :]
        return carry

    lax.fori_loop(0, chunks, body, 0)
    copy = pltpu.make_async_copy(final_ref.at[pl.ds(0, count)], out_hbm, sem)
    copy.start()
    copy.wait()


def local(sizes, cap, state, velocity, cells, slots, counts):
    sections, _, cx, cy, depth = velocity.shape
    count, width = state.shape
    moving = 8 * cap
    chunks = moving // LANES
    fields = sections * 3
    field = velocity.reshape(fields, cx, cy, depth)
    inner = cx * cy
    rim = 2 * cx + 2 * cy
    half = moving // 2
    base, merged, index, _, _ = pl.pallas_call(
        functools.partial(steps_kernel, sizes, cap),
        out_shape=(
            pltpu.VMEM((count, width), jnp.float32),
            pltpu.VMEM((moving, width), jnp.float32),
            pltpu.SMEM((sections, 2 * chunks, LANES), jnp.int32),
            pltpu.SMEM(counts.shape, jnp.int32),
            pltpu.SMEM((count // LANES, LANES), jnp.int32),
        ),
        in_specs=[ANY] * 5,
        out_specs=(VMEM, VMEM, SMEM, SMEM, SMEM),
        scratch_shapes=[
            pltpu.VMEM((count + (sections - 1) * moving, width), jnp.float32),
            pltpu.VMEM((sections, half, width), jnp.int32),
            pltpu.VMEM((sections, half, width), jnp.int32),
            pltpu.VMEM((8, count), jnp.float32),
            pltpu.VMEM(field.shape, field.dtype),
            pltpu.VMEM(cells.shape, jnp.int32),
            pltpu.VMEM(slots.shape, jnp.int32),
            pltpu.VMEM((sections, 2 * chunks, LANES), jnp.int32),
            pltpu.VMEM((count // LANES, LANES), jnp.int32),
            pltpu.VMEM((sections, count // LANES, LANES), jnp.int32),
            pltpu.VMEM((sections, chunks, LANES), jnp.int32),
            pltpu.VMEM((chunks, 8, LANES), jnp.int32),
            pltpu.VMEM((chunks, 8, LANES), jnp.float32),
            pltpu.VMEM((moving, width), jnp.float32),
            pltpu.VMEM((sections, 3 * depth, inner + 2 * LANES), jnp.bfloat16),
            pltpu.VMEM((2, fields, cx, depth), field.dtype),
            pltpu.VMEM((2, 4, 8, depth), jnp.float32),
            pltpu.VMEM((fields, rim, depth), field.dtype),
            pltpu.VMEM((2, 4, 8, depth), jnp.float32),
            pltpu.VMEM((2, 2, 3, cy, depth), field.dtype),
            pltpu.VMEM((2, 4, 8, depth), jnp.float32),
            pltpu.VMEM((3 * depth, 2 * LANES), jnp.bfloat16),
            pltpu.VMEM((chunks, 8, LANES), jnp.float32),
            pltpu.VMEM((chunks, 8, LANES), jnp.float32),
            pltpu.VMEM((sections, chunks, 8, LANES), jnp.float32),
            pltpu.VMEM((sections, 8, 8, LANES), jnp.float32),
            pltpu.SemaphoreType.DMA((7 + sections,)),
            pltpu.SemaphoreType.DMA((8 + 2 * sections,)),
            pltpu.SemaphoreType.DMA((8 + 2 * sections,)),
        ],
        compiler_params=pltpu.CompilerParams(collective_id=0, has_side_effects=True),
    )(state, field, cells, slots, counts)
    base, merged = (pltpu.with_memory_space_constraint(x, pltpu.VMEM) for x in (base, merged))
    index = pltpu.with_memory_space_constraint(index, pltpu.SMEM)
    return pl.pallas_call(
        functools.partial(last_kernel, cap),
        out_shape=jax.ShapeDtypeStruct((count, width), jnp.float32),
        in_specs=[VMEM, VMEM, SMEM],
        out_specs=ANY,
        scratch_shapes=[pltpu.VMEM((count + SPARE, width), jnp.float32), pltpu.SemaphoreType.DMA],
    )(base, merged, index)


def solution(mesh):
    return jax.shard_map(
        functools.partial(local, (mesh.shape["gx"], mesh.shape["gy"]), 64),
        mesh=mesh,
        in_specs=(
            P(("gx", "gy"), None),
            P(None, None, "gx", "gy", None),
            P(None, None, ("gx", "gy")),
            P(None, ("gx", "gy")),
            P(None, "gx", "gy", None),
        ),
        out_specs=P(("gx", "gy"), None),
        check_vma=False,
    )
```

```python
import functools

import jax
import jax.numpy as jnp
from jax import lax
from jax.experimental import pallas as pl
from jax.experimental.pallas import tpu as pltpu
from jax.sharding import PartitionSpec as P

GAMMA = (8.0 / 15.0, 5.0 / 12.0, 3.0 / 4.0)
ZETA = (0.0, -17.0 / 60.0, -5.0 / 12.0)
OFFSETS = ((1, 0), (-1, 0), (0, 1), (0, -1), (1, 1), (-1, -1), (1, -1), (-1, 1))
LANES = 128
FAR = ((0, 2), (0, -2))
CORNER_SLOT = (2, 0, 3, 1)
SPARE = 8
TOP = 65535.0
BLOCK = 512
MESH = pl.DeviceIdType.MESH
VMEM = pl.BlockSpec(memory_space=pltpu.VMEM)
SMEM = pl.BlockSpec(memory_space=pltpu.SMEM)
ANY = pl.BlockSpec(memory_space=pl.ANY)


def neighbour(offset, sizes):
    off_x, off_y = offset
    i, j = lax.axis_index("gx"), lax.axis_index("gy")
    return (lax.rem(i + off_x + sizes[0], sizes[0]), lax.rem(j + off_y + sizes[1], sizes[1]))


def send(offset, src, dst, sems, group, sizes):
    pltpu.make_async_remote_copy(
        src_ref=src,
        dst_ref=dst,
        send_sem=sems[0].at[group],
        recv_sem=sems[1].at[group],
        device_id=neighbour(offset, sizes),
        device_id_type=MESH,
    ).start()


def whole(everything, sems, group, sizes):
    return pltpu.make_async_remote_copy(
        src_ref=everything,
        dst_ref=everything,
        send_sem=sems[0].at[group],
        recv_sem=sems[1].at[group],
        device_id=neighbour(OFFSETS[0], sizes),
        device_id_type=MESH,
    )


def tile(x, k):
    return x[:, k * LANES : (k + 1) * LANES]


def spread_row(row):
    return jnp.broadcast_to(row, (8, LANES))


def select_lanes(tiles, where_, start):
    low, high = where_ & (LANES - 1), where_ >> 7
    out = start
    for k, source in enumerate(tiles):
        out = jnp.where(high == k, jnp.take_along_axis(source, low, axis=1), out)
    return out


def look_up(table, where_):
    low, high = spread_row(where_ & (LANES - 1)), spread_row(where_ >> 7)
    row = lax.broadcasted_iota(jnp.int32, (8, LANES), 0)
    best = jnp.zeros((8, LANES), jnp.int32)
    for g in range(table.shape[0] // 8):
        got = jnp.take_along_axis(table[8 * g : 8 * g + 8], low, axis=1)
        best = jnp.where(row + 8 * g == high, got, best)
    return jnp.max(best, axis=0, keepdims=True)


def cell_weights(size, cell, frac):
    spots = lax.broadcasted_iota(jnp.int32, (size, cell.shape[1]), 0)
    low, high = 1.0 - frac, frac
    inside = jnp.where(spots == cell, low, jnp.where(spots == cell + 1, high, 0.0))
    return inside, jnp.where(cell == -1, low, 0.0), jnp.where(cell == size - 1, high, 0.0)


def halves(value):
    high = value.astype(jnp.bfloat16)
    return high, (value - high.astype(jnp.float32)).astype(jnp.bfloat16)


def sum_depth(columns, wz):
    depth = wz.shape[0]
    return jnp.concatenate(
        [jnp.sum(columns[k * depth : (k + 1) * depth] * wz, axis=0, keepdims=True) for k in range(3)],
        axis=0,
    )


def multiply(plane, parts):
    total = jnp.dot(plane, parts[0], preferred_element_type=jnp.float32)
    for part in parts[1:]:
        total = total + jnp.dot(plane, part, preferred_element_type=jnp.float32)
    return total


def own_weights(wx, wy):
    return jnp.concatenate([wx[x : x + 1] * wy for x in range(wx.shape[0])], axis=0)


def rim_weights(wxs, wys):
    wx, wx_low, wx_high = wxs
    wy, wy_low, wy_high = wys
    rim = [wx_high * wy, wx_low * wy, wx * wy_high, wx * wy_low]
    rim += [wx_high * wy_high, wx_low * wy_low, wx_high * wy_low, wx_low * wy_high]
    filled = sum(part.shape[0] for part in rim)
    rim += [jnp.zeros((LANES - filled, wy.shape[1]), jnp.float32)]
    return jnp.concatenate(halves(jnp.concatenate(rim, axis=0)), axis=0)


def weights_of(dims, depth, head, cell):
    wxs = cell_weights(dims[0], cell[0:1], head[0:1])
    wys = cell_weights(dims[1], cell[1:2], head[1:2])
    wz, _, _ = cell_weights(depth, cell[2:3], head[2:3])
    return wxs, wys, wz


def advance(section, head, speed):
    moved = head[0:3] + GAMMA[section] * speed + ZETA[section] * head[3:6]
    return jnp.concatenate([moved, speed, jnp.ones((2, speed.shape[1]), jnp.float32)], axis=0)


def sample(section, dims, head, cell, plane_ref):
    inner = dims[0] * dims[1]
    wxs, wys, wz = weights_of(dims, plane_ref.shape[0] // 3, head, cell)
    columns = multiply(plane_ref[:, 0:inner], halves(own_weights(wxs[0], wys[0])))
    columns = columns + multiply(plane_ref[:, inner:], [rim_weights(wxs, wys)])
    return advance(section, head, sum_depth(columns, wz))


def unpack_cell(word):
    return jnp.concatenate([(word & 63) - 1, ((word >> 6) & 63) - 1, word >> 12], axis=0)


def sample_all(section, dims, cells_ref, head_ref, plane_ref):
    block = BLOCK

    for step in range(head_ref.shape[1] // block):
        span = slice(step * block, (step + 1) * block)
        head_ref[:, span] = sample(section, dims, head_ref[:, span], cells_ref[section, :, span], plane_ref)


def gather_rows(index_ref, source_ref, target_ref):
    for t in range(target_ref.shape[0]):
        target_ref[t : t + 1, :] = source_ref[pl.ds(index_ref[t // LANES, t % LANES], 1), :]


def encode(rows):
    lane = lax.broadcasted_iota(jnp.int32, rows.shape, 1)
    top = jnp.max(jnp.where(lane < 6, 0.0, rows), axis=1, keepdims=True)
    power = jnp.clip(jnp.floor(-jnp.log2(top)), 0.0, 100.0)
    code = jnp.minimum(rows * (jnp.exp2(power) * TOP) + 0.5, TOP)
    return jnp.where(lane < 6, power, code).astype(jnp.int32)


def decode(code):
    value = code.astype(jnp.float32)
    return value * (jnp.exp2(-value[:, 0:1]) * (1.0 / TOP))


def encode_rows(leave_ref, packed_ref):
    half = packed_ref.shape[0] // 8
    for r in range(8):
        first = encode(leave_ref[2 * half * r : 2 * half * r + half, :])
        second = encode(leave_ref[2 * half * r + half : 2 * half * (r + 1), :])
        packed_ref[half * r : half * (r + 1), :] = (first << 16) | second


def decode_rows(packed_ref, target_ref, start):
    half = packed_ref.shape[0] // 8
    for r in range(8):
        word = packed_ref[half * r : half * (r + 1), :]
        low = start + 2 * half * r
        target_ref[low : low + half, :] = decode((word >> 16) & 65535)
        target_ref[low + half : low + 2 * half, :] = decode(word & 65535)


def find_edges(fields, dims, v_ref, yface_ref, away_ref):
    cx, cy = dims
    inner = cx * cy
    row = lax.broadcasted_iota(jnp.int32, (2 * cx + 8, inner), 0)
    place = lax.broadcasted_iota(jnp.int32, (2 * cx + 8, inner), 1)
    want = jnp.where(row < cx, row * cy + cy - 1, (row - cx) * cy)
    for d, spot in enumerate((inner - 1, 0, (cx - 1) * cy, cy - 1)):
        want = jnp.where(row == 2 * cx + d, spot, want)
    pick = jnp.where(want == place, 1.0, 0.0).astype(jnp.bfloat16)
    for f in fields:
        edge = jnp.dot(pick, v_ref[f].reshape(inner, v_ref.shape[3]), preferred_element_type=jnp.float32)
        yface_ref[0, f] = edge[0:cx].astype(jnp.bfloat16)
        yface_ref[1, f] = edge[cx : 2 * cx].astype(jnp.bfloat16)
        group, line = (0, f) if f < 3 else (1, f - 3)
        for d in range(4):
            away_ref[group, d, line : line + 1, :] = edge[2 * cx + d : 2 * cx + d + 1]


def build_inside(section, dims, v_ref, plane_ref):
    inner = dims[0] * dims[1]
    depth = v_ref.shape[3]
    for k in range(3):
        own = v_ref[3 * section + k].reshape(inner, depth)
        plane_ref[pl.ds(k * depth, depth), 0:inner] = own.T


def build_rim(section, dims, halo_ref, corner_ref, plane_ref, with_plus=True):
    cx, cy = dims
    inner = cx * cy
    depth = halo_ref.shape[2]
    for k in range(3):
        f = 3 * section + k
        group, line = (0, f) if f < 3 else (1, f - 3)
        plus = halo_ref[f, 0:cy, :].astype(jnp.float32) if with_plus else jnp.zeros((cy, depth), jnp.float32)
        faces = [plus, halo_ref[f, cy:, :].astype(jnp.float32)]
        corners = [corner_ref[group, CORNER_SLOT[d], line : line + 1, :] for d in range(4)]
        if not with_plus:
            corners = [jnp.zeros((1, depth), jnp.float32) if d % 2 == 0 else corners[d] for d in range(4)]
        filler = jnp.zeros((LANES - 2 * cx - 2 * cy - 4, depth), jnp.float32)
        edge = jnp.concatenate(faces + corners + [filler], axis=0).T.astype(jnp.bfloat16)
        plane_ref[pl.ds(k * depth, depth), inner : inner + LANES] = edge
        plane_ref[pl.ds(k * depth, depth), inner + LANES :] = edge


def build_columns(dims, v_ref, face_ref, far_ref, column_ref):
    cx, cy = dims
    depth = v_ref.shape[3]
    for k in range(3):
        edge = []
        for side, x, above, below in ((0, 0, 1, 3), (1, cx - 1, 2, 0)):
            edge += [face_ref[1, side, k].astype(jnp.float32), v_ref[k, x].astype(jnp.float32)]
            edge += [face_ref[0, side, k].astype(jnp.float32), far_ref[0, above, k : k + 1, :]]
            edge += [jnp.zeros((LANES // 2 - 3 * cy - 2, depth), jnp.float32), far_ref[1, below, k : k + 1, :]]
        edge = jnp.concatenate(edge, axis=0).T.astype(jnp.bfloat16)
        column_ref[pl.ds(k * depth, depth), 0:LANES] = edge
        column_ref[pl.ds(k * depth, depth), LANES:] = edge


def finish_arrivals(dims, came, cap, column_ref, done_ref):
    cx, cy = dims
    half = LANES // 2
    crossed = [c for c in range(len(came)) if c != 1]
    head = jnp.concatenate([came[c] for c in crossed], axis=1)
    cell = unpack_cell(head[6:7].astype(jnp.int32))
    lanes = lax.broadcasted_iota(jnp.int32, (1, head.shape[1]), 1)
    odd = (lanes & cap) > 0
    shift = jnp.zeros((1, head.shape[1]), jnp.int32)
    for place, c in enumerate(crossed):
        for r in (2 * c, 2 * c + 1):
            here = (lanes >> 6) == 2 * place + r % 2
            shift = jnp.where(here, -cy * OFFSETS[r][1], shift)
    wx = jnp.where(odd, jnp.where(cell[0:1] == -1, 1.0 - head[0:1], 0.0), jnp.where(cell[0:1] == cx - 1, head[0:1], 0.0))
    base = jnp.where(odd, half, 0)
    first = base + ((cell[1:2] + shift + cy) & (half - 1))
    second = base + ((cell[1:2] + shift + cy + 1) & (half - 1))
    spots = lax.broadcasted_iota(jnp.int32, (LANES, head.shape[1]), 0)
    low, high = wx * (1.0 - head[1:2]), wx * head[1:2]
    weight = jnp.where(spots == first, low, jnp.where(spots == second, high, 0.0))
    wz, _, _ = cell_weights(column_ref.shape[0] // 3, cell[2:3], head[2:3])
    columns = multiply(column_ref[...], [jnp.concatenate(halves(weight), axis=0)])
    speed = head[3:6] + sum_depth(columns, wz)
    for place, c in enumerate(crossed):
        done_ref[c] = advance(0, tile(head, place), tile(speed, place))
    done_ref[1] = advance(0, came[1], came[1][3:6])


def plan(section, cap, count, slots_ref, counts_ref):
    moving = 8 * cap
    blocks = count // LANES
    slot = slots_ref[section : section + 1, 0:moving]
    lanes = lax.broadcasted_iota(jnp.int32, (1, moving), 1)
    limit = jnp.zeros((1, moving), jnp.int32)
    for r in range(8):
        limit = jnp.where(lanes >= r * cap, counts_ref[section, 0, 0, r], limit)
    taken = lax.rem(lanes, cap) < limit
    goal = jnp.where(taken, slot, count)
    value = jnp.where(taken, (lanes ^ cap) + 1, 0)
    low, high = slot & (LANES - 1), slot >> 7
    line = lax.broadcasted_iota(jnp.int32, (blocks, moving), 0)
    upper = jnp.where(line == high, (value >> 5).astype(jnp.float32), 0.0)
    lower = jnp.where(line == high, (value & 31).astype(jnp.float32), 0.0)
    left = jnp.concatenate([upper, lower], axis=0).astype(jnp.bfloat16)
    spots = lax.broadcasted_iota(jnp.int32, (LANES, moving), 0)
    right = jnp.where(spots == low, 1.0, 0.0).astype(jnp.bfloat16)
    both = lax.dot_general(left, right, (((1,), (1,)), ((), ())), preferred_element_type=jnp.float32)
    inverse = (both[0:blocks] * 32.0 + both[blocks:]).astype(jnp.int32)
    return slot, goal, inverse


def steps_kernel(
    sizes,
    cap,
    state_hbm,
    v_hbm,
    cells_hbm,
    slots_hbm,
    counts_hbm,
    base_ref,
    merged_ref,
    goal_ref,
    index_ref,
    counts_ref,
    places_ref,
    rows_ref,
    packed_ref,
    arrived_ref,
    head_ref,
    v_ref,
    cells_ref,
    slots_ref,
    staged_ref,
    final_ref,
    inverse_ref,
    from_ref,
    there_ref,
    own_ref,
    leave_ref,
    plane_ref,
    yface_ref,
    away_ref,
    halo_ref,
    corner_ref,
    face_ref,
    far_ref,
    column_ref,
    done_ref,
    late_ref,
    head_out_ref,
    head_in_ref,
    local_sem,
    send_sem,
    recv_sem,
):
    sems = (send_sem, recv_sem)
    sections, _, count = cells_ref.shape
    cx, cy = v_ref.shape[1], v_ref.shape[2]
    dims = (cx, cy)
    inner = cx * cy
    moving = 8 * cap
    chunks = moving // LANES
    blocks = count // LANES
    fields = 3 * sections
    starts = (0, cy, 2 * cy, 2 * cy + cx)
    widths = (cy, cy, cx, cx)

    barrier = pltpu.get_barrier_semaphore()
    for offset in OFFSETS + FAR:
        pl.semaphore_signal(barrier, inc=1, device_id=neighbour(offset, sizes), device_id_type=MESH)

    def fetch(k, src, dst):
        copy = pltpu.make_async_copy(src, dst, local_sem.at[k])
        copy.start()
        return copy

    load_first = fetch(0, v_hbm.at[pl.ds(0, 3)], v_ref.at[pl.ds(0, 3)])
    load_slots = fetch(1, slots_hbm, slots_ref)
    load_counts = fetch(2, counts_hbm, counts_ref)
    load_state = fetch(3, state_hbm, rows_ref.at[pl.ds(0, count)])
    load_cells = fetch(4, cells_hbm, cells_ref)
    load_rest = fetch(5, v_hbm.at[pl.ds(3, fields - 3)], v_ref.at[pl.ds(3, fields - 3)])

    spans = (pl.ds(0, 3), pl.ds(3, fields - 3))

    def send_halo(group):
        span = spans[group]
        for r in range(8):
            late = 2 if group == 0 and r in (1, 5, 7) else 0
            if r < 4:
                off_x, off_y = OFFSETS[r]
                src = v_ref.at[span, cx - 1 if off_x > 0 else 0] if off_x else yface_ref.at[r - 2, span]
                dst = halo_ref.at[span, pl.ds(starts[r ^ 1], widths[r ^ 1]), :]
                send(OFFSETS[r], src, dst, sems, 4 * group + late, sizes)
            else:
                src, dst = away_ref.at[group, r - 4], corner_ref.at[group, CORNER_SLOT[(r ^ 1) - 4]]
                send(OFFSETS[r], src, dst, sems, 4 * group + late + 1, sizes)
        if group:
            faces = whole(halo_ref.at[span], sems, 4, sizes)
            return [faces, whole(corner_ref.at[group], sems, 5, sizes)]
        early = whole(halo_ref.at[span, pl.ds(cy, 2 * cx + cy), :], sems, 0, sizes)
        late = whole(halo_ref.at[span, pl.ds(0, cy), :], sems, 2, sizes)
        corners = [whole(corner_ref.at[group, pl.ds(2 * part, 2)], sems, 2 * part + 1, sizes) for part in range(2)]
        return [early, corners[0], late, corners[1]]

    def send_columns():
        for r in (2, 3):
            for side, x in ((0, 0), (1, cx - 1)):
                send(OFFSETS[r], v_ref.at[spans[0], x], face_ref.at[(r ^ 1) - 2, side], sems, 6, sizes)
        for k, offset in enumerate(FAR):
            send(offset, away_ref.at[0], far_ref.at[1 - k], sems, 7, sizes)
        return [whole(face_ref, sems, 6, sizes), whole(far_ref, sems, 7, sizes)]

    load_first.wait()
    find_edges(range(3), dims, v_ref, yface_ref, away_ref)
    pl.semaphore_wait(barrier, len(OFFSETS + FAR))
    halos = [send_halo(0), send_columns()]

    load_slots.wait()
    load_counts.wait()
    slots, inverses = [], []
    table = lax.broadcasted_iota(jnp.int32, (blocks, LANES), 0) * LANES
    table = table + lax.broadcasted_iota(jnp.int32, (blocks, LANES), 1)
    places = []
    for section in range(sections):
        slot, goal, inverse = plan(section, cap, count, slots_ref, counts_ref)
        if section:
            packed = table * 1024 + inverses[-1]
            found = [look_up(packed, tile(slot, c)) for c in range(chunks)]
            for c in range(chunks):
                staged_ref[section, c : c + 1, :] = jnp.clip(found[c] >> 10, 0, count + section * moving - 1)
                from_ref[section, c : c + 1, :] = (found[c] & 1023) - 1
        else:
            for c in range(chunks):
                staged_ref[section, c : c + 1, :] = tile(slot, c)
        for c in range(chunks):
            staged_ref[section, chunks + c : chunks + c + 1, :] = tile(goal, c)
        places.append(fetch(6 + section, staged_ref.at[section], index_ref.at[section]))
        if section + 1 == sections:
            final_ref[...] = jnp.clip(table, 0, count + section * moving - 1)
            places.append(fetch(6 + sections, final_ref, places_ref))
            places.append(fetch(7 + sections, staged_ref.at[section], goal_ref))
        table = jnp.where(inverse > 0, inverse + (count + section * moving - 1), table)
        inverse_ref[section] = inverse - 1
        slots.append(slot)
        inverses.append(inverse)

    load_rest.wait()
    find_edges(range(3, fields), dims, v_ref, yface_ref, away_ref)
    halos.append(send_halo(1))

    def send_rows(section):
        places[section].wait()
        gather_rows(index_ref.at[section], rows_ref, leave_ref)
        encode_rows(leave_ref, packed_ref.at[section])
        half = cap // 2
        for r in range(8):
            span = pl.ds(r * half, half)
            send(OFFSETS[r], packed_ref.at[section, span], arrived_ref.at[section, span], sems, 8 + section, sizes)
        return [whole(arrived_ref.at[section], sems, 8 + section, sizes)]

    load_state.wait()
    carried = [send_rows(0)]
    for section in range(sections):
        build_inside(section, dims, v_ref, plane_ref.at[section])
    for b in range(blocks):
        head_ref[:, b * LANES : (b + 1) * LANES] = rows_ref[b * LANES : (b + 1) * LANES, :].T[0:8]

    load_cells.wait()
    line = lax.broadcasted_iota(jnp.int32, (8, LANES), 0)
    packed = []
    for b in range(blocks):
        span = slice(b * LANES, (b + 1) * LANES)
        both = jnp.zeros((8, LANES), jnp.int32)
        for section in range(sections):
            spot = cells_ref[section, :, span]
            word = (spot[0:1] + 1) + (spot[1:2] + 1) * 64 + spot[2:3] * 4096
            both = jnp.where(line == section, spread_row(word), both)
        packed.append(both)
    for c in range(chunks):
        where_ = spread_row(tile(slots[0], c))
        for section in range(1, sections):
            where_ = jnp.where(line == section, spread_row(tile(slots[section], c)), where_)
        there_ref[c] = select_lanes(packed, where_, jnp.zeros((8, LANES), jnp.int32))

    def pick_own(section):
        tiles = [head_ref[:, b * LANES : (b + 1) * LANES] for b in range(blocks)]
        for c in range(chunks):
            where_ = spread_row(slots_ref[section : section + 1, c * LANES : (c + 1) * LANES])
            own_ref[c] = select_lanes(tiles, where_, jnp.zeros((8, LANES), jnp.float32))

    def arrivals(section):
        first = lax.broadcasted_iota(jnp.int32, (8, LANES), 1) < cap
        return [
            jnp.where(first, head_in_ref[section, 2 * c], head_in_ref[section, 2 * c + 1]) for c in range(chunks)
        ]

    pick_own(0)
    heads = []
    for section in range(sections):
        group = 8 + sections + section
        word = jnp.concatenate([there_ref[c, section : section + 1, :] for c in range(chunks)], axis=1)
        cell = unpack_cell(word)
        if section == 0:
            head = jnp.concatenate([own_ref[c] for c in range(chunks)], axis=1)
            r = lax.broadcasted_iota(jnp.int32, (1, moving), 1) // cap
            plus = (r == 0) | (r == 4) | (r == 6)
            minus = (r == 1) | (r == 5) | (r == 7)
            wxs, wys, wz = weights_of(dims, v_ref.shape[3], head, cell)
            inside = plane_ref[0, :, 0:inner]
            columns = multiply(inside, halves(own_weights(wxs[0], wys[0])))
            none = jnp.zeros_like(wxs[2])
            lows = (wxs[0], jnp.where(minus, 0.0, wxs[1]), none)
            highs = (jnp.zeros_like(wxs[0]), none, jnp.where(plus, 0.0, wxs[2]))
            for copy in halos[0][0:2]:
                copy.wait_recv()
            build_rim(0, dims, halo_ref, corner_ref, plane_ref.at[0], with_plus=False)
            columns = columns + multiply(plane_ref[0, :, inner:], [rim_weights(lows, wys)])
            speed = sum_depth(columns, wz)
            tail = [word.astype(jnp.float32), jnp.ones((1, moving), jnp.float32)]
            message = jnp.concatenate([head[0:3], speed] + tail, axis=0)
            for c in range(chunks):
                head_out_ref[section, c] = tile(message, c)
            for r in (0, 4, 6):
                send(OFFSETS[r], head_out_ref.at[section, r // 2], head_in_ref.at[section, r], sems, group, sizes)
            for copy in halos[0][2:4]:
                copy.wait_recv()
            build_rim(0, dims, halo_ref, corner_ref, plane_ref.at[0])
            speed = speed + sum_depth(multiply(plane_ref[0, :, inner:], [rim_weights(highs, wys)]), wz)
            message = jnp.concatenate([head[0:3], speed] + tail, axis=0)
            for c in range(chunks):
                late_ref[c] = tile(message, c)
            for r in (1, 5, 7, 2, 3):
                send(OFFSETS[r], late_ref.at[r // 2], head_in_ref.at[section, r], sems, group, sizes)
        else:
            for copy in heads[section - 1]:
                copy.wait_recv()
            came = arrivals(section - 1)
            if section == 1:
                finish_arrivals(dims, came, cap, column_ref, done_ref)
                came = [done_ref[c] for c in range(chunks)]
            leaving = [
                select_lanes(came, spread_row(from_ref[section, c : c + 1, :]), own_ref[c]) for c in range(chunks)
            ]
            leaving = sample(section, dims, jnp.concatenate(leaving, axis=1), cell, plane_ref.at[section])
            for c in range(chunks):
                head_out_ref[section, c] = tile(leaving, c)
            for r in range(8):
                send(OFFSETS[r], head_out_ref.at[section, r // 2], head_in_ref.at[section, r], sems, group, sizes)
        heads.append([whole(head_in_ref.at[section], sems, group, sizes)])

        if section:
            came = [done_ref[c] for c in range(chunks)] if section == 1 else arrivals(section - 1)
            place_arrivals(section - 1, came, inverse_ref, head_ref)
        sample_all(section, dims, cells_ref, head_ref, plane_ref.at[section])
        if section + 1 < sections:
            pick_own(section + 1)
            if section == 0:
                for copy in halos[1] + halos[2]:
                    copy.wait_recv()
                build_columns(dims, v_ref, face_ref, far_ref, column_ref)
                for later in range(1, sections):
                    build_rim(later, dims, halo_ref, corner_ref, plane_ref.at[later])
            for copy in carried[section]:
                copy.wait_recv()
            decode_rows(arrived_ref.at[section], rows_ref, count + section * moving)
            carried.append(send_rows(section + 1))

    places[sections].wait()
    places[sections + 1].wait()
    gather_rows(places_ref, rows_ref, base_ref)
    for b in range(blocks):
        span = slice(b * LANES, (b + 1) * LANES)
        base_ref[span, :] = merge_head(head_ref[:, span], base_ref[span, :])
    for copy in carried[sections - 1]:
        copy.wait_recv()
    decode_rows(arrived_ref.at[sections - 1], merged_ref, 0)
    for copies in halos + carried + heads[:-1]:
        for copy in copies:
            copy.wait_send()
    for copy in heads[sections - 1]:
        copy.wait_recv()
    for c, came in enumerate(arrivals(sections - 1)):
        span = slice(c * LANES, (c + 1) * LANES)
        merged_ref[span, :] = merge_head(came, merged_ref[span, :])
    for copy in heads[sections - 1]:
        copy.wait_send()


def merge_head(head, rows):
    lane = lax.broadcasted_iota(jnp.int32, rows.shape, 1)
    full = jnp.concatenate([head, jnp.zeros((rows.shape[1] - 8, LANES), jnp.float32)], axis=0)
    return jnp.where(lane < 6, full.T, rows)


def place_arrivals(section, came, inverse_ref, head_ref):
    for b in range(head_ref.shape[1] // LANES):
        span = slice(b * LANES, (b + 1) * LANES)
        where_ = spread_row(inverse_ref[section, b : b + 1, :])
        head_ref[:, span] = select_lanes(came, where_, head_ref[:, span])


def last_kernel(cap, base_ref, merged_ref, goal_ref, out_hbm, final_ref, sem):
    count = out_hbm.shape[0]
    chunks = 8 * cap // LANES
    final_ref[0:count, :] = base_ref[...]

    for t in range(8 * cap):
        goal = goal_ref[chunks + t // LANES, t % LANES]
        final_ref[pl.ds(goal, 1), :] = merged_ref[(t ^ cap) : (t ^ cap) + 1, :]
    copy = pltpu.make_async_copy(final_ref.at[pl.ds(0, count)], out_hbm, sem)
    copy.start()
    copy.wait()


def local(sizes, cap, state, velocity, cells, slots, counts):
    sections, _, cx, cy, depth = velocity.shape
    count, width = state.shape
    moving = 8 * cap
    chunks = moving // LANES
    fields = sections * 3
    field = velocity.reshape(fields, cx, cy, depth)
    inner = cx * cy
    rim = 2 * cx + 2 * cy
    half = moving // 2
    base, merged, goal = pl.pallas_call(
        functools.partial(steps_kernel, sizes, cap),
        out_shape=(
            pltpu.VMEM((count, width), jnp.float32),
            pltpu.VMEM((moving, width), jnp.float32),
            pltpu.SMEM((2 * chunks, LANES), jnp.int32),
        ),
        in_specs=[ANY] * 5,
        out_specs=(VMEM, VMEM, SMEM),
        scratch_shapes=[
            pltpu.SMEM((sections, 2 * chunks, LANES), jnp.int32),
            pltpu.SMEM(counts.shape, jnp.int32),
            pltpu.SMEM((count // LANES, LANES), jnp.int32),
            pltpu.VMEM((count + (sections - 1) * moving, width), jnp.float32),
            pltpu.VMEM((sections, half, width), jnp.int32),
            pltpu.VMEM((sections, half, width), jnp.int32),
            pltpu.VMEM((8, count), jnp.float32),
            pltpu.VMEM(field.shape, field.dtype),
            pltpu.VMEM(cells.shape, jnp.int32),
            pltpu.VMEM(slots.shape, jnp.int32),
            pltpu.VMEM((sections, 2 * chunks, LANES), jnp.int32),
            pltpu.VMEM((count // LANES, LANES), jnp.int32),
            pltpu.VMEM((sections, count // LANES, LANES), jnp.int32),
            pltpu.VMEM((sections, chunks, LANES), jnp.int32),
            pltpu.VMEM((chunks, 8, LANES), jnp.int32),
            pltpu.VMEM((chunks, 8, LANES), jnp.float32),
            pltpu.VMEM((moving, width), jnp.float32),
            pltpu.VMEM((sections, 3 * depth, inner + 2 * LANES), jnp.bfloat16),
            pltpu.VMEM((2, fields, cx, depth), field.dtype),
            pltpu.VMEM((2, 4, 8, depth), jnp.float32),
            pltpu.VMEM((fields, rim, depth), field.dtype),
            pltpu.VMEM((2, 4, 8, depth), jnp.float32),
            pltpu.VMEM((2, 2, 3, cy, depth), field.dtype),
            pltpu.VMEM((2, 4, 8, depth), jnp.float32),
            pltpu.VMEM((3 * depth, 2 * LANES), jnp.bfloat16),
            pltpu.VMEM((chunks, 8, LANES), jnp.float32),
            pltpu.VMEM((chunks, 8, LANES), jnp.float32),
            pltpu.VMEM((sections, chunks, 8, LANES), jnp.float32),
            pltpu.VMEM((sections, 8, 8, LANES), jnp.float32),
            pltpu.SemaphoreType.DMA((8 + sections,)),
            pltpu.SemaphoreType.DMA((8 + 2 * sections,)),
            pltpu.SemaphoreType.DMA((8 + 2 * sections,)),
        ],
        compiler_params=pltpu.CompilerParams(collective_id=0, has_side_effects=True),
    )(state, field, cells, slots, counts)
    base, merged = (pltpu.with_memory_space_constraint(x, pltpu.VMEM) for x in (base, merged))
    goal = pltpu.with_memory_space_constraint(goal, pltpu.SMEM)
    return pl.pallas_call(
        functools.partial(last_kernel, cap),
        out_shape=jax.ShapeDtypeStruct((count, width), jnp.float32),
        in_specs=[VMEM, VMEM, SMEM],
        out_specs=ANY,
        scratch_shapes=[pltpu.VMEM((count + SPARE, width), jnp.float32), pltpu.SemaphoreType.DMA],
    )(base, merged, goal)


def solution(mesh):
    return jax.shard_map(
        functools.partial(local, (mesh.shape["gx"], mesh.shape["gy"]), 64),
        mesh=mesh,
        in_specs=(
            P(("gx", "gy"), None),
            P(None, None, "gx", "gy", None),
            P(None, None, ("gx", "gy")),
            P(None, ("gx", "gy")),
            P(None, "gx", "gy", None),
        ),
        out_specs=P(("gx", "gy"), None),
        check_vma=False,
    )
```
